32 devices in a mesh: dp: 4 (over y, x), mp: 8 (over z, core).
Axes of the slice: x: 2, y: 2, z: 4, core: 2. Of those that a mesh axis runs over, the one named last changes fastest.
Arguments:
- tokens: bfloat16 [4, 1024, 5120], P('dp', 'mp'), may hold values from -6 to 6
- ln_gain: float32 [5120], replicated, may hold values from 0.1 to 1.9
- ln_bias: float32 [5120], replicated, may hold values from -3 to 3
- w_qkv: bfloat16 [5120, 3, 4096], P(None, None, 'mp'), may hold values from -0.15625 to 0.15625
- w_out: bfloat16 [4096, 5120], P('mp'), may hold values from -0.09375 to 0.09375
- grad_partial: bfloat16 [4, 4096, 5120], P('dp', 'mp'), may hold values from -6 to 6
Outputs:
- mixed: bfloat16 [4, 1024, 5120], P('dp', 'mp')
- grad_sum: float32 [4096, 5120], P('mp')
The draws below stay inside these ranges and needn't reach their ends.
All inputs are finite; a program needn't handle non-finite values.
Results may differ from the reference program's by a relative error of at most 0.014.
The reference program's roundings to bfloat16 on the way (of `normed`, `qkv`, `attn` and `context`) count: a program that leaves them out, or rounds other values in their place, can miss the bound.
Values may be sent and summed in bfloat16 or wider, within the bound.
A program may use at most 192 MiB of HBM per device.

```python
import jax
import jax.numpy as jnp
from jax import lax

D = 5120
HEAD = 128
HEADS = 32
SEQ = 128
IMG = 8
INNER = 4096
TOKENS = 1024
GROUPS = 4
N_MP = 8


def levels(key, shape, cuts, smallest, top_value):
    loudness = 1.0
    for dim, blocks in cuts:
        heights = jax.random.uniform(jax.random.fold_in(jax.random.fold_in(key, 6), dim), (blocks,), jnp.float32, smallest / len(cuts), top_value / len(cuts))
        loudness = loudness * jnp.repeat(jnp.exp(heights), shape[dim] // blocks).reshape((-1,) + (1,) * (len(shape) - 1 - dim))
    return loudness


def noise(rng, shape, scale, bound, shards=(), dtype=jnp.bfloat16):
    gain = levels(rng, shape, shards, -0.22, 0.18) if shards else 1.0
    drawn = jax.random.normal(rng, shape, jnp.float32) * scale * gain
    return jnp.minimum(jnp.maximum(drawn, -bound), bound).astype(dtype)


def setup_inputs(seed: int = 0) -> dict:
    streams_of = jax.random.split(jax.random.key(seed), 7)
    tokens = noise(streams_of[0], (GROUPS, TOKENS, D), 1.0, 6.0, ((0, 4), (1, 8)))
    ln_gain = jnp.clip(1.0 + 0.18 * jax.random.normal(streams_of[1], (D,), jnp.float32), 0.1, 1.9)
    ln_bias = noise(streams_of[2], (D,), 0.5, 3.0, (), jnp.float32)
    w_qkv = noise(streams_of[3], (D, 3, INNER), (D // 4) ** -0.5, 0.15625, ((2, 8),))
    w_out = noise(streams_of[4], (INNER, D), INNER ** -0.5, 0.09375, ((0, 8),))
    grad_partial = noise(streams_of[5], (GROUPS, INNER, D), 1.0, 6.0, ((0, 4), (1, 8)))
    return {"tokens": tokens, "ln_gain": ln_gain, "ln_bias": ln_bias, "w_qkv": w_qkv, "w_out": w_out, "grad_partial": grad_partial}


def layer_norm(rows, ln_gain, ln_bias):
    values = rows.astype(jnp.float32)
    center = lax.optimization_barrier(jnp.mean(values, axis=-1, keepdims=True))
    spread = lax.optimization_barrier(jnp.mean((values - center) * (values - center), axis=-1, keepdims=True))
    return ((values - center) * lax.rsqrt(spread + 1e-06) * ln_gain + ln_bias).astype(jnp.bfloat16)

def one_group(rows, ln_gain, ln_bias, w_qkv, w_out):
    normed = layer_norm(rows, ln_gain, ln_bias)
    qkv = jnp.dot(normed, w_qkv.reshape(D, 3 * INNER), preferred_element_type=jnp.float32).astype(jnp.bfloat16)
    query = qkv[:, :INNER].reshape(IMG, SEQ, HEADS, HEAD).astype(jnp.float32)
    keys = qkv[:, INNER:2 * INNER].reshape(IMG, SEQ, HEADS, HEAD).astype(jnp.float32)
    values = qkv[:, 2 * INNER:].reshape(IMG, SEQ, HEADS, HEAD).astype(jnp.float32)
    scores = jnp.einsum('bqhd,bkhd->bhqk', query, keys) * HEAD ** (-0.5)
    scaled = scores - lax.optimization_barrier(jnp.max(scores, axis=-1, keepdims=True))
    expsc = jnp.exp(scaled)
    attn = (expsc / lax.optimization_barrier(jnp.sum(expsc, axis=-1, keepdims=True))).astype(jnp.bfloat16)
    context = jnp.einsum('bhqk,bkhd->bqhd', attn.astype(jnp.float32), values).astype(jnp.bfloat16)
    context = context.reshape(TOKENS, INNER)
    width = INNER // N_MP

    def add_group(index, total):
        start = (index * width).astype(jnp.int32)
        cols = lax.dynamic_slice_in_dim(context, start, width, 1)
        wrows = lax.dynamic_slice_in_dim(w_out, start, width, 0)
        partial_sum = jnp.dot(cols, wrows, preferred_element_type=jnp.float32).astype(jnp.bfloat16)
        partial_sum = lax.optimization_barrier(partial_sum)
        return total + partial_sum.astype(jnp.float32)
    proj = lax.fori_loop(0, N_MP, add_group, jnp.zeros((TOKENS, D), jnp.float32))
    return (rows.astype(jnp.float32) + proj).astype(jnp.bfloat16)

def reference(tokens, ln_gain, ln_bias, w_qkv, w_out, grad_partial):
    mixed = lax.map(lambda rows: one_group(rows, ln_gain, ln_bias, w_qkv, w_out), tokens)
    grad_sum = lax.optimization_barrier(jnp.sum(grad_partial.astype(jnp.float32), axis=0))
    return (mixed, grad_sum)
```

```python
import functools

import jax
import jax.numpy as jnp
from jax import lax
from jax.experimental import pallas as pl
from jax.experimental.pallas import tpu as pltpu
from jax.sharding import PartitionSpec as P

HEAD = 128
SEQ = 128
NORM_ROWS = 16
MESH = pl.DeviceIdType.MESH


def pieces_of(half):
    return next(p for p in (5, 4) if half % (p * 128) == 0)


def kernel(
    n,
    tok_hbm,
    gain,
    bias,
    wq_hbm,
    wo_hbm,
    out_hbm,
    wq,
    wo,
    tok,
    tok_mate,
    blocks,
    theirs,
    stage,
    chain,
    fin,
    out,
    qkv,
    ctx,
    load_sem,
    own_send,
    own_recv,
    up_send,
    up_recv,
    dn_send,
    dn_recv,
    mx_send,
    mx_recv,
    mp_send,
    mp_recv,
    fin_send,
    fin_recv,
):
    chips = n // 2
    slots = 2 * chips
    me = lax.axis_index("mp")
    c = me // 2
    s = me % 2
    mate = c * 2 + 1 - s
    above = me + 2
    below = me - 2
    high = chips - 1 - c
    up = jnp.minimum(high, 1)
    dn = jnp.minimum(c, 1)
    rows, width = tok.shape
    half = width // 2
    pieces = pieces_of(half)
    wide = half // pieces
    inner = wo.shape[0]
    f32 = jnp.float32
    bf16 = jnp.bfloat16

    def remote(src, dst, send, recv, target):
        return pltpu.make_async_remote_copy(
            src_ref=src,
            dst_ref=dst,
            send_sem=send,
            recv_sem=recv,
            device_id={"mp": target},
            device_id_type=MESH,
        )

    def side(h):
        return pl.ds(pl.multiple_of(h * half, 128), half)

    def cols(h, p):
        return pl.ds(pl.multiple_of(h * half + p * wide, 128), wide)

    def sub(p):
        return pl.ds(pl.multiple_of(p * wide, 128), wide)

    def gather_above(a):
        first = a < high
        return jnp.where(first, 2 * (c + 1 + a), 2 * (c + 2 * high - a) + 1)

    def gather_below(a):
        first = a < c
        return jnp.where(first, 2 * (c - 1 - a), 2 * (a - c) + 1)

    def sum_into_up(chip, j):
        first = j < chips + chip
        return jnp.where(first, 2 * (j - chip), 2 * (chip - 1 + slots - j) + 1)

    def sum_into_dn(chip, j):
        mirror = chips - 1 - chip
        first = j < chips + mirror
        t = jnp.where(first, j - mirror, mirror - 1 + slots - j)
        return 2 * (chips - 1 - t) + jnp.where(first, 0, 1)

    def chain_up(chip, j):
        return j - 2 * chip

    def chain_dn(chip, j):
        return 2 * (chips - chip) + j - 2 * (chips - 1 - chip)

    load_t = pltpu.make_async_copy(tok_hbm, tok, load_sem.at[0])
    load_q = pltpu.make_async_copy(wq_hbm, wq, load_sem.at[1])
    load_o = pltpu.make_async_copy(wo_hbm, wo, load_sem.at[2])
    store = pltpu.make_async_copy(out, out_hbm, load_sem.at[3])
    load_t.start()
    load_q.start()
    load_o.start()

    barrier = pltpu.get_barrier_semaphore()
    pl.semaphore_signal(barrier, inc=1, device_id={"mp": mate}, device_id_type=MESH)

    @pl.when(up > 0)
    def _():
        pl.semaphore_signal(barrier, inc=1, device_id={"mp": above}, device_id_type=MESH)

    @pl.when(dn > 0)
    def _():
        pl.semaphore_signal(barrier, inc=1, device_id={"mp": below}, device_id_type=MESH)

    load_t.wait()

    def norm(r, carry):
        here = pl.ds(pl.multiple_of(r * NORM_ROWS, NORM_ROWS), NORM_ROWS)
        values = tok[here, :].astype(f32)
        center = jnp.mean(values, axis=-1, keepdims=True)
        values = values - center
        spread = jnp.mean(values * values, axis=-1, keepdims=True)
        blocks[me, here, :] = (values * lax.rsqrt(spread + 1e-06) * gain[...] + bias[...]).astype(bf16)
        return carry

    lax.fori_loop(0, rows // NORM_ROWS, norm, 0)

    pl.semaphore_wait(barrier, 1 + up + dn)

    def own(slot, h, i):
        at = blocks.at[slot, :, side(h)]
        return remote(at, at, own_send.at[i], own_recv.at[i], mate)

    def raw(h):
        return remote(tok.at[:, side(h)], tok_mate, own_send.at[2], own_recv.at[2], mate)

    own(me, 1 - s, 0).start()
    own(me, s, 1).start()
    raw(1 - s).start()

    def hop_up(slot, j, p):
        at = blocks.at[slot, :, cols(s, p)]
        return remote(at, at, up_send.at[j], up_recv.at[j, p], above)

    def hop_dn(slot, j, p):
        at = blocks.at[slot, :, cols(s, p)]
        return remote(at, at, dn_send.at[j], dn_recv.at[j, p], below)

    def add_up(slot, j, p):
        return remote(
            theirs.at[slot, :, sub(p)],
            chain.at[chain_up(c + 1, j), :, sub(p)],
            up_send.at[j],
            up_recv.at[j, p],
            above,
        )

    def add_dn(slot, j, p):
        return remote(
            theirs.at[slot, :, sub(p)],
            chain.at[chain_dn(c - 1, j), :, sub(p)],
            dn_send.at[j],
            dn_recv.at[j, p],
            below,
        )

    def to_mate(slot, p):
        at = blocks.at[slot, :, cols(s, p)]
        return remote(at, at, mx_send.at[slot], mx_recv.at[slot], mate)

    def from_mate(slot):
        at = blocks.at[slot, :, side(1 - s)]
        return remote(at, at, mx_send.at[slot], mx_recv.at[slot], mate)

    def share(k, slot):
        return remote(stage.at[k], theirs.at[slot], mp_send.at[k], mp_recv.at[slot], mate)

    @pl.when(s == 1)
    def _():
        own(2 * c, s, 0).wait_recv()

    @pl.when(up > 0)
    def _():
        for p in range(pieces):
            hop_up(2 * c, 0, p).start()

    @pl.when(dn > 0)
    def _():
        for p in range(pieces):
            hop_dn(2 * c, 0, p).start()

    @pl.when(s == 0)
    def _():
        own(2 * c + 1, s, 0).wait_recv()

    @pl.when(dn == 0)
    def _():
        chain[chain_up(c, 2 * c), :, :] = jnp.zeros((rows, half), bf16)
        chain[chain_up(c, slots - 1), :, :] = jnp.zeros((rows, half), bf16)

    @pl.when(up == 0)
    def _():
        chain[chain_dn(c, 2 * high), :, :] = jnp.zeros((rows, half), bf16)
        chain[chain_dn(c, slots - 1), :, :] = jnp.zeros((rows, half), bf16)

    own(mate, 1 - s, 1).wait_recv()
    raw(s).wait_recv()
    own(me, 1 - s, 0).wait_send()
    own(me, s, 1).wait_send()
    raw(1 - s).wait_send()
    load_q.wait()
    load_o.wait()

    def project(slot):
        def one(which, carry):
            qkv[which, :, :] = jnp.dot(
                blocks[slot], wq[which], preferred_element_type=f32
            ).astype(bf16)
            return carry

        lax.fori_loop(0, 3, one, 0)

    def attend():
        for image in range(rows // SEQ):
            here = slice(image * SEQ, (image + 1) * SEQ)
            for h in range(inner // HEAD):
                lanes = slice(h * HEAD, (h + 1) * HEAD)
                scores = lax.dot_general(
                    qkv[0, here, lanes],
                    qkv[1, here, lanes],
                    (((1,), (1,)), ((), ())),
                    preferred_element_type=f32,
                ) * HEAD ** (-0.5)
                expsc = jnp.exp(scores - jnp.max(scores, axis=-1, keepdims=True))
                attn = (expsc / jnp.sum(expsc, axis=-1, keepdims=True)).astype(bf16)
                ctx[here, lanes] = jnp.dot(
                    attn, qkv[2, here, lanes], preferred_element_type=f32
                ).astype(bf16)

    block = half // 2

    def output(slot, k):
        for i in range(2):
            at = pl.ds(pl.multiple_of((1 - s) * half + i * block, 128), block)
            stage[k, :, i * block : (i + 1) * block] = jnp.dot(
                ctx[...], wo[:, at], preferred_element_type=f32
            ).astype(bf16)
        share(k, slot).start()
        for i in range(2):
            at = pl.ds(pl.multiple_of(s * half + i * block, 128), block)
            to = pl.ds(pl.multiple_of((1 - s) * half + i * block, 128), block)
            blocks[slot, :, to] = jnp.dot(
                ctx[...], wo[:, at], preferred_element_type=f32
            ).astype(bf16)

    def mine(slot, p):
        return blocks[slot, :, cols(1 - s, p)].astype(f32) + theirs[slot, :, sub(p)].astype(f32)

    def finish(slot, p, foreign):
        value = (
            mine(slot, p)
            + chain[chain_up(c, jnp.where(slot % 2 == 0, 2 * c, slots - 1)), :, sub(p)].astype(f32)
            + chain[chain_dn(c, jnp.where(slot % 2 == 0, 2 * high, slots - 1)), :, sub(p)].astype(f32)
        )
        if foreign:
            fin[:, sub(p)] = (tok_mate[:, sub(p)].astype(f32) + value).astype(bf16)
            give(p).start()
        else:
            out[:, cols(s, p)] = (tok[:, cols(s, p)].astype(f32) + value).astype(bf16)

    def give(p):
        return remote(fin.at[:, sub(p)], out.at[:, cols(s, p)], fin_send.at[p], fin_recv.at[p], mate)

    def take(p):
        return remote(fin.at[:, sub(p)], out.at[:, cols(1 - s, p)], fin_send.at[p], fin_recv.at[p], mate)

    top = 1 - up

    def candidate(j, k):
        a = j - 1
        has_above = jnp.minimum(jnp.maximum(2 * high - a, 0), 1)
        has_below = jnp.minimum(jnp.maximum(2 * c - a, 0), 1)
        from_above = jnp.where(k == 0, 1 - top, 0)
        from_below = jnp.where(k == 0, top, 1 - top)
        later = from_above * has_above + from_below * has_below
        exists = jnp.where(j == 0, 1, later)
        slot = jnp.where(from_above == 1, gather_above(a), gather_below(a))
        return exists, jnp.where(j == 0, 2 * c + k, slot)

    def tick(j, p):
        k = p // 2
        exists, slot = candidate(j, k)
        active = jnp.where(p < 4, exists, 0)

        @pl.when(active * (1 - p % 2) > 0)
        def _():
            @pl.when(j > 0)
            def _():
                from_mate(slot).wait_recv()

            project(slot)

        @pl.when(active * (p % 2) > 0)
        def _():
            attend()
            output(slot, k)

        last = jnp.where(j == slots - 1, 1, 0)

        @pl.when(last * jnp.where(p == 0, 1, 0) > 0)
        def _():
            share(0, 2 * c).wait_recv()
            share(0, 2 * c + 1).wait_recv()
            for ab in range(2):
                @pl.when(s == ab)
                def _():
                    def one(q, carry):
                        finish(2 * c, q, ab == 1)
                        return carry

                    lax.fori_loop(0, pieces, one, 0)

        @pl.when(dn > 0)
        def _():
            @pl.when(j < 2 * c)
            def _():
                image = gather_below(j)
                hop_up(image, j, p).wait_recv()

                @pl.when(up > 0)
                def _():
                    hop_up(image, j + 1, p).start()

                to_mate(image, p).start()

            @pl.when(j >= 2 * c)
            def _():
                image = sum_into_up(c, j)
                at = chain_up(c, j)
                remote(
                    theirs.at[image, :, sub(p)],
                    chain.at[at, :, sub(p)],
                    up_send.at[j],
                    up_recv.at[j, p],
                    above,
                ).wait_recv()

                @pl.when(image >= 2 * c + 2)
                def _():
                    @pl.when(p == 0)
                    def _():
                        share(0, image).wait_recv()

                    theirs[image, :, sub(p)] = (
                        mine(image, p) + chain[at, :, sub(p)].astype(f32)
                    ).astype(bf16)
                    add_up(image, j + 1, p).start()

        @pl.when(up > 0)
        def _():
            @pl.when(j < 2 * high)
            def _():
                image = gather_above(j)
                hop_dn(image, j, p).wait_recv()

                @pl.when(dn > 0)
                def _():
                    hop_dn(image, j + 1, p).start()

                to_mate(image, p).start()

            @pl.when(j >= 2 * high)
            def _():
                image = sum_into_dn(c, j)
                at = chain_dn(c, j)
                remote(
                    theirs.at[image, :, sub(p)],
                    chain.at[at, :, sub(p)],
                    dn_send.at[j],
                    dn_recv.at[j, p],
                    below,
                ).wait_recv()

                @pl.when(image < 2 * c)
                def _():
                    @pl.when(p == 0)
                    def _():
                        share(0, image).wait_recv()

                    theirs[image, :, sub(p)] = (
                        mine(image, p) + chain[at, :, sub(p)].astype(f32)
                    ).astype(bf16)
                    add_dn(image, j + 1, p).start()

        @pl.when(up * jnp.where(p == 0, 1, 0) * jnp.where(j == 2 * c, 1, 0) > 0)
        def _():
            for q in range(pieces):
                hop_up(2 * c + 1, 2 * c + 1, q).start()

        @pl.when(dn * jnp.where(p == 0, 1, 0) * jnp.where(j == 2 * high, 1, 0) > 0)
        def _():
            for q in range(pieces):
                hop_dn(2 * c + 1, 2 * high + 1, q).start()

        begin = jnp.where(p == 3, 1, 0) * jnp.minimum(j, 1) * (1 - last)

        @pl.when(begin * (1 - dn) * up > 0)
        def _():
            image = sum_into_up(c + 1, j + 1)
            share(0, image).wait_recv()

            def one(q, carry):
                theirs[image, :, sub(q)] = mine(image, q).astype(bf16)
                add_up(image, j + 1, q).start()
                return carry

            lax.fori_loop(0, pieces, one, 0)

        @pl.when(begin * (1 - up) * dn > 0)
        def _():
            image = sum_into_dn(c - 1, j + 1)
            share(0, image).wait_recv()

            def one(q, carry):
                theirs[image, :, sub(q)] = mine(image, q).astype(bf16)
                add_dn(image, j + 1, q).start()
                return carry

            lax.fori_loop(0, pieces, one, 0)

        for ab in range(2):
            @pl.when(last * jnp.where(s == ab, 1, 0) > 0)
            def _():
                finish(2 * c + 1, p, ab == 0)

        @pl.when(p == pieces - 1)
        def _():
            for b in range(2):
                there, image = candidate(j, b)

                @pl.when(there > 0)
                def _():
                    share(b, image).wait_send()

    def slot_loop(j, carry):
        def piece_loop(p, inside):
            tick(j, p)
            return inside

        return lax.fori_loop(0, pieces, piece_loop, carry)

    lax.fori_loop(0, slots, slot_loop, 0)

    for p in range(pieces):
        take(p).wait_recv()
    store.start()

    def drain(j, carry):
        @pl.when(up > 0)
        def _():
            remote(
                blocks.at[0, :, side(s)], blocks.at[0, :, side(s)], up_send.at[j], up_recv.at[0, 0], above
            ).wait_send()

        @pl.when(dn > 0)
        def _():
            remote(
                blocks.at[0, :, side(s)], blocks.at[0, :, side(s)], dn_send.at[j], dn_recv.at[0, 0], below
            ).wait_send()

        @pl.when(j // 2 != c)
        def _():
            from_mate(j).wait_send()

        return carry

    lax.fori_loop(0, slots, drain, 0)
    for p in range(pieces):
        give(p).wait_send()
    store.wait()


def body(n, tokens, ln_gain, ln_bias, w_qkv, w_out, grad_partial):
    local_rows = tokens[0]
    rows, width = local_rows.shape
    inner = w_out.shape[0]
    chips = n // 2
    slots = 2 * chips
    half = width // 2
    pieces = pieces_of(half)
    dma = pltpu.SemaphoreType.DMA
    flops = 2 * rows * n * width * inner * 4
    vmem = pl.BlockSpec(memory_space=pltpu.VMEM)
    hbm = pl.BlockSpec(memory_space=pl.ANY)
    mixed = pl.pallas_call(
        functools.partial(kernel, n),
        out_shape=jax.ShapeDtypeStruct((rows, width), jnp.bfloat16),
        in_specs=[hbm, vmem, vmem, hbm, hbm],
        out_specs=hbm,
        scratch_shapes=[
            pltpu.VMEM((3, width, inner), jnp.bfloat16),
            pltpu.VMEM((inner, width), jnp.bfloat16),
            pltpu.VMEM((rows, width), jnp.bfloat16),
            pltpu.VMEM((rows, half), jnp.bfloat16),
            pltpu.VMEM((n, rows, width), jnp.bfloat16),
            pltpu.VMEM((n, rows, half), jnp.bfloat16),
            pltpu.VMEM((2, rows, half), jnp.bfloat16),
            pltpu.VMEM((slots + 2, rows, half), jnp.bfloat16),
            pltpu.VMEM((rows, half), jnp.bfloat16),
            pltpu.VMEM((rows, width), jnp.bfloat16),
            pltpu.VMEM((3, rows, inner), jnp.bfloat16),
            pltpu.VMEM((rows, inner), jnp.bfloat16),
            dma((4,)),
            dma((3,)),
            dma((3,)),
            dma((slots,)),
            dma((slots, pieces)),
            dma((slots,)),
            dma((slots, pieces)),
            dma((n,)),
            dma((n,)),
            dma((2,)),
            dma((n,)),
            dma((pieces,)),
            dma((pieces,)),
        ],
        compiler_params=pltpu.CompilerParams(
            collective_id=0, has_side_effects=True, vmem_limit_bytes=66_000_000
        ),
        cost_estimate=pl.CostEstimate(
            flops=flops * 8, bytes_accessed=300_000_000, transcendentals=0
        ),
    )(
        local_rows,
        ln_gain.reshape(1, width),
        ln_bias.reshape(1, width),
        jnp.transpose(w_qkv, (1, 0, 2)),
        w_out,
    )[None]
    grad_sum = lax.psum(grad_partial[0], "dp").astype(jnp.float32)
    return (mixed, grad_sum)


def solution(mesh):
    placed = (
        P("dp", "mp", None),
        P(),
        P(),
        P(None, None, "mp"),
        P("mp", None),
        P("dp", "mp", None),
    )
    return jax.shard_map(
        functools.partial(body, mesh.shape["mp"]),
        mesh=mesh,
        in_specs=placed,
        out_specs=(P("dp", "mp", None), P("mp", None)),
        check_vma=False,
    )
```

```python
import functools

import jax
import jax.numpy as jnp
from jax import lax
from jax.experimental import pallas as pl
from jax.experimental.pallas import tpu as pltpu
from jax.sharding import PartitionSpec as P

HEAD = 128
SEQ = 128
NORM_ROWS = 16
MESH = pl.DeviceIdType.MESH


def pieces_of(half):
    return next(p for p in (5, 4) if half % (p * 128) == 0)


def kernel(
    n,
    groups,
    tok_hbm,
    gain,
    bias,
    wq_hbm,
    wo_hbm,
    grad_hbm,
    out,
    total,
    wq,
    wo,
    tok,
    tok_mate,
    blocks,
    theirs,
    stage,
    chain,
    fin,
    qkv,
    ctx,
    income,
    load_sem,
    own_send,
    own_recv,
    up_send,
    up_recv,
    dn_send,
    dn_recv,
    mx_send,
    mx_recv,
    mp_send,
    mp_recv,
    fin_send,
    fin_recv,
    rs_send,
    rs_recv,
    ag_send,
    ag_recv,
):
    bits = groups.bit_length() - 1
    assert groups == 1 << bits
    group = lax.axis_index("dp")
    chips = n // 2
    slots = 2 * chips
    me = lax.axis_index("mp")
    c = me // 2
    s = me % 2
    mate = c * 2 + 1 - s
    above = me + 2
    below = me - 2
    high = chips - 1 - c
    up = jnp.minimum(high, 1)
    dn = jnp.minimum(c, 1)
    rows, width = tok.shape
    half = width // 2
    pieces = pieces_of(half)
    wide = half // pieces
    inner = wo.shape[0]
    f32 = jnp.float32
    bf16 = jnp.bfloat16

    def remote(src, dst, send, recv, target):
        return pltpu.make_async_remote_copy(
            src_ref=src,
            dst_ref=dst,
            send_sem=send,
            recv_sem=recv,
            device_id={"mp": target},
            device_id_type=MESH,
        )

    def side(h):
        return pl.ds(pl.multiple_of(h * half, 128), half)

    def cols(h, p):
        return pl.ds(pl.multiple_of(h * half + p * wide, 128), wide)

    def sub(p):
        return pl.ds(pl.multiple_of(p * wide, 128), wide)

    def gather_above(a):
        first = a < high
        return jnp.where(first, 2 * (c + 1 + a), 2 * (c + 2 * high - a) + 1)

    def gather_below(a):
        first = a < c
        return jnp.where(first, 2 * (c - 1 - a), 2 * (a - c) + 1)

    def sum_into_up(chip, j):
        first = j < chips + chip
        return jnp.where(first, 2 * (j - chip), 2 * (chip - 1 + slots - j) + 1)

    def sum_into_dn(chip, j):
        mirror = chips - 1 - chip
        first = j < chips + mirror
        t = jnp.where(first, j - mirror, mirror - 1 + slots - j)
        return 2 * (chips - 1 - t) + jnp.where(first, 0, 1)

    def chain_up(chip, j):
        return j - 2 * chip

    def chain_dn(chip, j):
        return 2 * (chips - chip) + j - 2 * (chips - 1 - chip)

    load_t = pltpu.make_async_copy(tok_hbm, tok, load_sem.at[0])
    load_q = pltpu.make_async_copy(wq_hbm, wq, load_sem.at[1])
    load_o = pltpu.make_async_copy(wo_hbm, wo, load_sem.at[2])
    load_t.start()
    load_q.start()
    load_o.start()

    grows = grad_hbm.shape[0] // 2

    def partner(h, i):
        bit = 1 << (i if h == 0 else bits - 1 - i)
        side_of = (group // bit) % 2
        return group + bit * (1 - 2 * side_of), side_of

    def region(h, i):
        base = h * grows
        size = grows
        for step in range(i + 1):
            size = size // 2
            if step < i:
                base = base + partner(h, step)[1] * size
        keep = partner(h, i)[1]
        return base + keep * size, base + (1 - keep) * size, size

    offset = [0]
    for step in range(bits):
        offset.append(offset[-1] + (grows >> (step + 1)))

    def span(base, size):
        return pl.ds(pl.multiple_of(base, 16), size)

    def scatter(h, i):
        _, away, size = region(h, i)
        if i == 0:
            source = grad_hbm.at[span(away, size), :]
        else:
            source = income.at[h, span(offset[i - 1] + away - region(h, i - 1)[0], size), :]
        return pltpu.make_async_remote_copy(
            src_ref=source,
            dst_ref=income.at[h, offset[i] : offset[i] + size, :],
            send_sem=rs_send.at[h, i],
            recv_sem=rs_recv.at[h, i],
            device_id={"dp": partner(h, i)[0]},
            device_id_type=MESH,
        )

    def collect(h, i):
        keep, _, size = region(h, i)
        at = total.at[span(keep, size), :]
        return pltpu.make_async_remote_copy(
            src_ref=at,
            dst_ref=at,
            send_sem=ag_send.at[h, i],
            recv_sem=ag_recv.at[h, i],
            device_id={"dp": partner(h, i)[0]},
            device_id_type=MESH,
        )

    def collected(h, i):
        _, away, size = region(h, i)
        at = total.at[span(away, size), :]
        return pltpu.make_async_remote_copy(
            src_ref=at,
            dst_ref=at,
            send_sem=ag_send.at[h, i],
            recv_sem=ag_recv.at[h, i],
            device_id={"dp": partner(h, i)[0]},
            device_id_type=MESH,
        )

    def load_g(h):
        keep, _, size = region(h, 0)
        return pltpu.make_async_copy(
            grad_hbm.at[span(keep, size), :], total.at[span(keep, size), :], load_sem.at[3 + h]
        )

    for h in range(2):
        load_g(h).start()

    def grad_event(e):
        for h in range(2):
            if e < bits:
                if e == 0:
                    load_g(h).wait()
                scatter(h, e).wait_recv()
                keep, _, size = region(h, e)

                def add(base, count, leaves):
                    def one(r, carry):
                        here = span(base + r * 16, 16)
                        there = span(offset[e] + base - keep + r * 16, 16)
                        both = total[here, :].astype(f32) + income[h, there, :].astype(f32)
                        if leaves:
                            income[h, there, :] = both.astype(bf16)
                        else:
                            total[here, :] = both.astype(bf16)
                        return carry

                    lax.fori_loop(0, count // 16, one, 0)

                if e + 1 < bits:
                    stay, leave, count = region(h, e + 1)
                    add(leave, count, True)
                    scatter(h, e + 1).start()
                    add(stay, count, False)
                else:
                    add(keep, size, False)
                    collect(h, e).start()
            else:
                i = 2 * bits - 1 - e
                collected(h, i).wait_recv()
                if i > 0:
                    collect(h, i - 1).start()


    times = []
    at_tick = 0
    for e in range(2 * bits):
        step = e if e < bits else 2 * bits - 1 - e
        lines = (grows >> (step + 1)) * width
        at_tick += -(-lines // (rows * wide)) + 1
        times.append(min(at_tick, slots * pieces - 2 * bits + e))

    barrier = pltpu.get_barrier_semaphore()
    pl.semaphore_signal(barrier, inc=1, device_id={"mp": mate}, device_id_type=MESH)

    @pl.when(up > 0)
    def _():
        pl.semaphore_signal(barrier, inc=1, device_id={"mp": above}, device_id_type=MESH)

    @pl.when(dn > 0)
    def _():
        pl.semaphore_signal(barrier, inc=1, device_id={"mp": below}, device_id_type=MESH)

    for i in range(bits):
        pl.semaphore_signal(
            barrier, inc=1, device_id={"dp": partner(0, i)[0]}, device_id_type=MESH
        )

    load_t.wait()

    def norm(r, carry):
        here = pl.ds(pl.multiple_of(r * NORM_ROWS, NORM_ROWS), NORM_ROWS)
        values = tok[here, :].astype(f32)
        center = jnp.mean(values, axis=-1, keepdims=True)
        values = values - center
        spread = jnp.mean(values * values, axis=-1, keepdims=True)
        blocks[me, here, :] = (values * lax.rsqrt(spread + 1e-06) * gain[...] + bias[...]).astype(bf16)
        return carry

    lax.fori_loop(0, rows // NORM_ROWS, norm, 0)

    pl.semaphore_wait(barrier, 1 + up + dn + bits)

    def own(slot, h, i):
        at = blocks.at[slot, :, side(h)]
        return remote(at, at, own_send.at[i], own_recv.at[i], mate)

    def raw(h):
        return remote(tok.at[:, side(h)], tok_mate, own_send.at[2], own_recv.at[2], mate)

    own(me, 1 - s, 0).start()
    own(me, s, 1).start()
    raw(1 - s).start()

    def hop_up(slot, j, p):
        at = blocks.at[slot, :, cols(s, p)]
        return remote(at, at, up_send.at[j], up_recv.at[j, p], above)

    def hop_dn(slot, j, p):
        at = blocks.at[slot, :, cols(s, p)]
        return remote(at, at, dn_send.at[j], dn_recv.at[j, p], below)

    def add_up(slot, j, p):
        return remote(
            theirs.at[slot, :, sub(p)],
            chain.at[chain_up(c + 1, j), :, sub(p)],
            up_send.at[j],
            up_recv.at[j, p],
            above,
        )

    def add_dn(slot, j, p):
        return remote(
            theirs.at[slot, :, sub(p)],
            chain.at[chain_dn(c - 1, j), :, sub(p)],
            dn_send.at[j],
            dn_recv.at[j, p],
            below,
        )

    def to_mate(slot, p):
        at = blocks.at[slot, :, cols(s, p)]
        return remote(at, at, mx_send.at[slot], mx_recv.at[slot], mate)

    def from_mate(slot):
        at = blocks.at[slot, :, side(1 - s)]
        return remote(at, at, mx_send.at[slot], mx_recv.at[slot], mate)

    def share(k, slot):
        return remote(stage.at[k], theirs.at[slot], mp_send.at[k], mp_recv.at[slot], mate)

    @pl.when(s == 1)
    def _():
        own(2 * c, s, 0).wait_recv()

    @pl.when(up > 0)
    def _():
        for p in range(pieces):
            hop_up(2 * c, 0, p).start()

    @pl.when(dn > 0)
    def _():
        for p in range(pieces):
            hop_dn(2 * c, 0, p).start()

    for h in range(2):
        scatter(h, 0).start()

    @pl.when(s == 0)
    def _():
        own(2 * c + 1, s, 0).wait_recv()

    @pl.when(dn == 0)
    def _():
        chain[chain_up(c, 2 * c), :, :] = jnp.zeros((rows, half), bf16)
        chain[chain_up(c, slots - 1), :, :] = jnp.zeros((rows, half), bf16)

    @pl.when(up == 0)
    def _():
        chain[chain_dn(c, 2 * high), :, :] = jnp.zeros((rows, half), bf16)
        chain[chain_dn(c, slots - 1), :, :] = jnp.zeros((rows, half), bf16)

    own(mate, 1 - s, 1).wait_recv()
    raw(s).wait_recv()
    own(me, 1 - s, 0).wait_send()
    own(me, s, 1).wait_send()
    raw(1 - s).wait_send()
    load_q.wait()
    load_o.wait()

    def project(slot):
        def one(which, carry):
            qkv[which, :, :] = jnp.dot(
                blocks[slot], wq[which], preferred_element_type=f32
            ).astype(bf16)
            return carry

        lax.fori_loop(0, 3, one, 0)

    def attend():
        for image in range(rows // SEQ):
            here = slice(image * SEQ, (image + 1) * SEQ)
            for h in range(inner // HEAD):
                lanes = slice(h * HEAD, (h + 1) * HEAD)
                scores = lax.dot_general(
                    qkv[0, here, lanes],
                    qkv[1, here, lanes],
                    (((1,), (1,)), ((), ())),
                    preferred_element_type=f32,
                ) * HEAD ** (-0.5)
                expsc = jnp.exp(scores - jnp.max(scores, axis=-1, keepdims=True))
                attn = (expsc / jnp.sum(expsc, axis=-1, keepdims=True)).astype(bf16)
                ctx[here, lanes] = jnp.dot(
                    attn, qkv[2, here, lanes], preferred_element_type=f32
                ).astype(bf16)

    block = half // 2

    def output(slot, k):
        for i in range(2):
            at = pl.ds(pl.multiple_of((1 - s) * half + i * block, 128), block)
            stage[k, :, i * block : (i + 1) * block] = jnp.dot(
                ctx[...], wo[:, at], preferred_element_type=f32
            ).astype(bf16)
        share(k, slot).start()
        for i in range(2):
            at = pl.ds(pl.multiple_of(s * half + i * block, 128), block)
            to = pl.ds(pl.multiple_of((1 - s) * half + i * block, 128), block)
            blocks[slot, :, to] = jnp.dot(
                ctx[...], wo[:, at], preferred_element_type=f32
            ).astype(bf16)

    def mine(slot, p):
        return blocks[slot, :, cols(1 - s, p)].astype(f32) + theirs[slot, :, sub(p)].astype(f32)

    def finish(slot, p, foreign):
        value = (
            mine(slot, p)
            + chain[chain_up(c, jnp.where(slot % 2 == 0, 2 * c, slots - 1)), :, sub(p)].astype(f32)
            + chain[chain_dn(c, jnp.where(slot % 2 == 0, 2 * high, slots - 1)), :, sub(p)].astype(f32)
        )
        if foreign:
            fin[:, sub(p)] = (tok_mate[:, sub(p)].astype(f32) + value).astype(bf16)
            give(p).start()
        else:
            out[:, cols(s, p)] = (tok[:, cols(s, p)].astype(f32) + value).astype(bf16)

    def give(p):
        return remote(fin.at[:, sub(p)], out.at[:, cols(s, p)], fin_send.at[p], fin_recv.at[p], mate)

    def take(p):
        return remote(fin.at[:, sub(p)], out.at[:, cols(1 - s, p)], fin_send.at[p], fin_recv.at[p], mate)

    top = 1 - up

    def candidate(j, k):
        a = j - 1
        has_above = jnp.minimum(jnp.maximum(2 * high - a, 0), 1)
        has_below = jnp.minimum(jnp.maximum(2 * c - a, 0), 1)
        from_above = jnp.where(k == 0, 1 - top, 0)
        from_below = jnp.where(k == 0, top, 1 - top)
        later = from_above * has_above + from_below * has_below
        exists = jnp.where(j == 0, 1, later)
        slot = jnp.where(from_above == 1, gather_above(a), gather_below(a))
        return exists, jnp.where(j == 0, 2 * c + k, slot)

    def tick(j, p):
        k = p // 2
        exists, slot = candidate(j, k)
        active = jnp.where(p < 4, exists, 0)

        @pl.when(active * (1 - p % 2) > 0)
        def _():
            @pl.when(j > 0)
            def _():
                from_mate(slot).wait_recv()

            project(slot)

        @pl.when(active * (p % 2) > 0)
        def _():
            attend()
            output(slot, k)

        last = jnp.where(j == slots - 1, 1, 0)

        @pl.when(last * jnp.where(p == 0, 1, 0) > 0)
        def _():
            share(0, 2 * c).wait_recv()
            share(0, 2 * c + 1).wait_recv()
            for ab in range(2):
                @pl.when(s == ab)
                def _():
                    def one(q, carry):
                        finish(2 * c, q, ab == 1)
                        return carry

                    lax.fori_loop(0, pieces, one, 0)

        @pl.when(dn > 0)
        def _():
            @pl.when(j < 2 * c)
            def _():
                image = gather_below(j)
                hop_up(image, j, p).wait_recv()

                @pl.when(up > 0)
                def _():
                    hop_up(image, j + 1, p).start()

                to_mate(image, p).start()

            @pl.when(j >= 2 * c)
            def _():
                image = sum_into_up(c, j)
                at = chain_up(c, j)
                remote(
                    theirs.at[image, :, sub(p)],
                    chain.at[at, :, sub(p)],
                    up_send.at[j],
                    up_recv.at[j, p],
                    above,
                ).wait_recv()

                @pl.when(image >= 2 * c + 2)
                def _():
                    @pl.when(p == 0)
                    def _():
                        share(0, image).wait_recv()

                    theirs[image, :, sub(p)] = (
                        mine(image, p) + chain[at, :, sub(p)].astype(f32)
                    ).astype(bf16)
                    add_up(image, j + 1, p).start()

        @pl.when(up > 0)
        def _():
            @pl.when(j < 2 * high)
            def _():
                image = gather_above(j)
                hop_dn(image, j, p).wait_recv()

                @pl.when(dn > 0)
                def _():
                    hop_dn(image, j + 1, p).start()

                to_mate(image, p).start()

            @pl.when(j >= 2 * high)
            def _():
                image = sum_into_dn(c, j)
                at = chain_dn(c, j)
                remote(
                    theirs.at[image, :, sub(p)],
                    chain.at[at, :, sub(p)],
                    dn_send.at[j],
                    dn_recv.at[j, p],
                    below,
                ).wait_recv()

                @pl.when(image < 2 * c)
                def _():
                    @pl.when(p == 0)
                    def _():
                        share(0, image).wait_recv()

                    theirs[image, :, sub(p)] = (
                        mine(image, p) + chain[at, :, sub(p)].astype(f32)
                    ).astype(bf16)
                    add_dn(image, j + 1, p).start()

        @pl.when(up * jnp.where(p == 0, 1, 0) * jnp.where(j == 2 * c, 1, 0) > 0)
        def _():
            for q in range(pieces):
                hop_up(2 * c + 1, 2 * c + 1, q).start()

        @pl.when(dn * jnp.where(p == 0, 1, 0) * jnp.where(j == 2 * high, 1, 0) > 0)
        def _():
            for q in range(pieces):
                hop_dn(2 * c + 1, 2 * high + 1, q).start()

        begin = jnp.where(p == 3, 1, 0) * jnp.minimum(j, 1) * (1 - last)

        @pl.when(begin * (1 - dn) * up > 0)
        def _():
            image = sum_into_up(c + 1, j + 1)
            share(0, image).wait_recv()

            def one(q, carry):
                theirs[image, :, sub(q)] = mine(image, q).astype(bf16)
                add_up(image, j + 1, q).start()
                return carry

            lax.fori_loop(0, pieces, one, 0)

        @pl.when(begin * (1 - up) * dn > 0)
        def _():
            image = sum_into_dn(c - 1, j + 1)
            share(0, image).wait_recv()

            def one(q, carry):
                theirs[image, :, sub(q)] = mine(image, q).astype(bf16)
                add_dn(image, j + 1, q).start()
                return carry

            lax.fori_loop(0, pieces, one, 0)

        for ab in range(2):
            @pl.when(last * jnp.where(s == ab, 1, 0) > 0)
            def _():
                finish(2 * c + 1, p, ab == 0)

        for e, when in enumerate(times):
            @pl.when(j * pieces + p == when)
            def _():
                grad_event(e)

        @pl.when(p == pieces - 1)
        def _():
            for b in range(2):
                there, image = candidate(j, b)

                @pl.when(there > 0)
                def _():
                    share(b, image).wait_send()

    def slot_loop(j, carry):
        def piece_loop(p, inside):
            tick(j, p)
            return inside

        return lax.fori_loop(0, pieces, piece_loop, carry)

    lax.fori_loop(0, slots, slot_loop, 0)

    for p in range(pieces):
        take(p).wait_recv()

    def drain(j, carry):
        @pl.when(up > 0)
        def _():
            remote(
                blocks.at[0, :, side(s)], blocks.at[0, :, side(s)], up_send.at[j], up_recv.at[0, 0], above
            ).wait_send()

        @pl.when(dn > 0)
        def _():
            remote(
                blocks.at[0, :, side(s)], blocks.at[0, :, side(s)], dn_send.at[j], dn_recv.at[0, 0], below
            ).wait_send()

        @pl.when(j // 2 != c)
        def _():
            from_mate(j).wait_send()

        return carry

    lax.fori_loop(0, slots, drain, 0)
    for p in range(pieces):
        give(p).wait_send()
    for h in range(2):
        for i in range(bits):
            scatter(h, i).wait_send()
            collect(h, i).wait_send()


def spread(mixed, total, mixed_hbm, total_hbm, wide, sem):
    parts = wide.shape[0]
    rows = wide.shape[1]
    first = pltpu.make_async_copy(mixed, mixed_hbm, sem.at[parts])
    first.start()

    def put(i):
        at = pl.ds(pl.multiple_of(i * rows, 8), rows)
        return pltpu.make_async_copy(wide.at[i], total_hbm.at[at, :], sem.at[i])

    def one(i, carry):
        at = pl.ds(pl.multiple_of(i * rows, 8), rows)
        wide[i, :, :] = total[at, :].astype(jnp.float32)
        put(i).start()
        return carry

    lax.fori_loop(0, parts, one, 0)

    def done(i, carry):
        put(i).wait()
        return carry

    lax.fori_loop(0, parts, done, 0)
    first.wait()


def body(n, groups, tokens, ln_gain, ln_bias, w_qkv, w_out, grad_partial):
    local_rows = tokens[0]
    rows, width = local_rows.shape
    inner = w_out.shape[0]
    grows = grad_partial.shape[1]
    chips = n // 2
    slots = 2 * chips
    bits = groups.bit_length() - 1
    half = width // 2
    pieces = pieces_of(half)
    dma = pltpu.SemaphoreType.DMA
    flops = 2 * rows * n * width * inner * 4
    vmem = pl.BlockSpec(memory_space=pltpu.VMEM)
    hbm = pl.BlockSpec(memory_space=pl.ANY)
    bf16 = jnp.bfloat16
    results = (rows + grows) * width * 2
    income = sum(grows >> (i + 2) for i in range(bits))
    mixed, total = pl.pallas_call(
        functools.partial(kernel, n, groups),
        out_shape=(pltpu.VMEM((rows, width), bf16), pltpu.VMEM((grows, width), bf16)),
        in_specs=[hbm, vmem, vmem, hbm, hbm, hbm],
        out_specs=(vmem, vmem),
        scratch_shapes=[
            pltpu.VMEM((3, width, inner), bf16),
            pltpu.VMEM((inner, width), bf16),
            pltpu.VMEM((rows, width), bf16),
            pltpu.VMEM((rows, half), bf16),
            pltpu.VMEM((n, rows, width), bf16),
            pltpu.VMEM((n, rows, half), bf16),
            pltpu.VMEM((2, rows, half), bf16),
            pltpu.VMEM((slots + 2, rows, half), bf16),
            pltpu.VMEM((rows, half), bf16),
            pltpu.VMEM((3, rows, inner), bf16),
            pltpu.VMEM((rows, inner), bf16),
            pltpu.VMEM((2, income, width), bf16),
            dma((5,)),
            dma((3,)),
            dma((3,)),
            dma((slots,)),
            dma((slots, pieces)),
            dma((slots,)),
            dma((slots, pieces)),
            dma((n,)),
            dma((n,)),
            dma((2,)),
            dma((n,)),
            dma((pieces,)),
            dma((pieces,)),
            dma((2, bits)),
            dma((2, bits)),
            dma((2, bits)),
            dma((2, bits)),
        ],
        compiler_params=pltpu.CompilerParams(
            collective_id=0, has_side_effects=True, vmem_limit_bytes=66_900_000 - results
        ),
        cost_estimate=pl.CostEstimate(
            flops=flops * 8, bytes_accessed=300_000_000, transcendentals=0
        ),
    )(
        local_rows,
        ln_gain.reshape(1, width),
        ln_bias.reshape(1, width),
        jnp.transpose(w_qkv, (1, 0, 2)),
        w_out,
        grad_partial[0],
    )
    parts = grows // 32
    mixed, grad_sum = pl.pallas_call(
        spread,
        out_shape=(
            jax.ShapeDtypeStruct((rows, width), bf16),
            jax.ShapeDtypeStruct((grows, width), jnp.float32),
        ),
        in_specs=[vmem, vmem],
        out_specs=(hbm, hbm),
        scratch_shapes=[
            pltpu.VMEM((parts, grows // parts, width), jnp.float32),
            dma((parts + 1,)),
        ],
        compiler_params=pltpu.CompilerParams(vmem_limit_bytes=grows * width * 4 + 2_000_000),
        cost_estimate=pl.CostEstimate(
            flops=grows * width, bytes_accessed=grows * width * 6, transcendentals=0
        ),
    )(mixed, total)
    return (mixed[None], grad_sum)


def solution(mesh):
    placed = (
        P("dp", "mp", None),
        P(),
        P(),
        P(None, None, "mp"),
        P("mp", None),
        P("dp", "mp", None),
    )
    return jax.shard_map(
        functools.partial(body, mesh.shape["mp"], mesh.shape["dp"]),
        mesh=mesh,
        in_specs=placed,
        out_specs=(P("dp", "mp", None), P("mp", None)),
        check_vma=False,
    )
```

```python
import functools

import jax
import jax.numpy as jnp
from jax import lax
from jax.experimental import pallas as pl
from jax.experimental.pallas import tpu as pltpu
from jax.sharding import PartitionSpec as P

HEAD = 128
SEQ = 128
NORM_ROWS = 16
MESH = pl.DeviceIdType.MESH


def pieces_of(half):
    return next(p for p in (4, 5) if half % (p * 128) == 0)


def kernel(
    n,
    groups,
    tok_hbm,
    gain,
    bias,
    wq_hbm,
    wo_hbm,
    grad_hbm,
    out,
    total,
    wq,
    wo,
    tok,
    tok_mate,
    blocks,
    theirs,
    stage,
    chain,
    fin,
    qkv,
    ctx,
    income,
    load_sem,
    own_send,
    own_recv,
    up_send,
    up_recv,
    dn_send,
    dn_recv,
    mx_send,
    mx_recv,
    mp_send,
    mp_recv,
    fin_send,
    fin_recv,
    rs_send,
    rs_recv,
    ag_send,
    ag_recv,
):
    bits = groups.bit_length() - 1
    assert groups == 1 << bits
    group = lax.axis_index("dp")
    chips = n // 2
    slots = 2 * chips
    me = lax.axis_index("mp")
    c = me // 2
    s = me % 2
    mate = c * 2 + 1 - s
    above = me + 2
    below = me - 2
    high = chips - 1 - c
    up = jnp.minimum(high, 1)
    dn = jnp.minimum(c, 1)
    rows, width = tok.shape
    half = width // 2
    pieces = pieces_of(half)
    wide = half // pieces
    inner = wo.shape[0]
    f32 = jnp.float32
    bf16 = jnp.bfloat16

    def remote(src, dst, send, recv, target):
        return pltpu.make_async_remote_copy(
            src_ref=src,
            dst_ref=dst,
            send_sem=send,
            recv_sem=recv,
            device_id={"mp": target},
            device_id_type=MESH,
        )

    def side(h):
        return pl.ds(pl.multiple_of(h * half, 128), half)

    def cols(h, p):
        return pl.ds(pl.multiple_of(h * half + p * wide, 128), wide)

    def sub(p):
        return pl.ds(pl.multiple_of(p * wide, 128), wide)

    def gather_above(a):
        first = a < high
        return jnp.where(first, 2 * (c + 1 + a), 2 * (c + 2 * high - a) + 1)

    def gather_below(a):
        first = a < c
        return jnp.where(first, 2 * (c - 1 - a), 2 * (a - c) + 1)

    def sum_into_up(chip, j):
        first = j < chips + chip
        return jnp.where(first, 2 * (j - chip), 2 * (chip - 1 + slots - j) + 1)

    def sum_into_dn(chip, j):
        mirror = chips - 1 - chip
        first = j < chips + mirror
        t = jnp.where(first, j - mirror, mirror - 1 + slots - j)
        return 2 * (chips - 1 - t) + jnp.where(first, 0, 1)

    def chain_up(chip, j):
        return j - 2 * chip

    def chain_dn(chip, j):
        return 2 * (chips - chip) + j - 2 * (chips - 1 - chip)

    load_t = pltpu.make_async_copy(tok_hbm, tok, load_sem.at[0])
    load_q = pltpu.make_async_copy(wq_hbm, wq, load_sem.at[1])
    load_o = pltpu.make_async_copy(wo_hbm, wo, load_sem.at[2])
    load_t.start()

    grows = grad_hbm.shape[0] // 2

    def partner(h, i):
        bit = 1 << (i if h == 0 else bits - 1 - i)
        side_of = (group // bit) % 2
        return group + bit * (1 - 2 * side_of), side_of

    def region(h, i):
        base = h * grows
        size = grows
        for step in range(i + 1):
            size = size // 2
            if step < i:
                base = base + partner(h, step)[1] * size
        keep = partner(h, i)[1]
        return base + keep * size, base + (1 - keep) * size, size

    offset = [0]
    for step in range(bits):
        offset.append(offset[-1] + (grows >> (step + 1)))

    def span(base, size):
        return pl.ds(pl.multiple_of(base, 16), size)

    def scatter(h, i):
        _, away, size = region(h, i)
        if i == 0:
            source = grad_hbm.at[span(away, size), :]
        else:
            source = income.at[h, span(offset[i - 1] + away - region(h, i - 1)[0], size), :]
        return pltpu.make_async_remote_copy(
            src_ref=source,
            dst_ref=income.at[h, offset[i] : offset[i] + size, :],
            send_sem=rs_send.at[h, i],
            recv_sem=rs_recv.at[h, i],
            device_id={"dp": partner(h, i)[0]},
            device_id_type=MESH,
        )

    def collect(h, i):
        keep, _, size = region(h, i)
        at = total.at[span(keep, size), :]
        return pltpu.make_async_remote_copy(
            src_ref=at,
            dst_ref=at,
            send_sem=ag_send.at[h, i],
            recv_sem=ag_recv.at[h, i],
            device_id={"dp": partner(h, i)[0]},
            device_id_type=MESH,
        )

    def collected(h, i):
        _, away, size = region(h, i)
        at = total.at[span(away, size), :]
        return pltpu.make_async_remote_copy(
            src_ref=at,
            dst_ref=at,
            send_sem=ag_send.at[h, i],
            recv_sem=ag_recv.at[h, i],
            device_id={"dp": partner(h, i)[0]},
            device_id_type=MESH,
        )

    def load_g(h):
        keep, _, size = region(h, 0)
        return pltpu.make_async_copy(
            grad_hbm.at[span(keep, size), :], total.at[span(keep, size), :], load_sem.at[3 + h]
        )

    def grad_event(e):
        for h in range(2):
            if e < bits:
                if e == 0:
                    load_g(h).wait()
                scatter(h, e).wait_recv()
                keep, _, size = region(h, e)

                def add(base, count, leaves):
                    def one(r, carry):
                        here = span(base + r * 16, 16)
                        there = span(offset[e] + base - keep + r * 16, 16)
                        both = total[here, :].astype(f32) + income[h, there, :].astype(f32)
                        if leaves:
                            income[h, there, :] = both.astype(bf16)
                        else:
                            total[here, :] = both.astype(bf16)
                        return carry

                    lax.fori_loop(0, count // 16, one, 0)

                if e + 1 < bits:
                    stay, leave, count = region(h, e + 1)
                    add(leave, count, True)
                    scatter(h, e + 1).start()
                    add(stay, count, False)
                else:
                    add(keep, size, False)
                    collect(h, e).start()
            else:
                i = 2 * bits - 1 - e
                collected(h, i).wait_recv()
                if i > 0:
                    collect(h, i - 1).start()


    times = []
    at_tick = 0
    for e in range(2 * bits):
        step = e if e < bits else 2 * bits - 1 - e
        lines = (grows >> (step + 1)) * width
        at_tick += -(-lines // (rows * wide)) + 1
        times.append(min(at_tick, slots * pieces - 2 * bits + e))

    barrier = pltpu.get_barrier_semaphore()
    pl.semaphore_signal(barrier, inc=1, device_id={"mp": mate}, device_id_type=MESH)

    @pl.when(up > 0)
    def _():
        pl.semaphore_signal(barrier, inc=1, device_id={"mp": above}, device_id_type=MESH)

    @pl.when(dn > 0)
    def _():
        pl.semaphore_signal(barrier, inc=1, device_id={"mp": below}, device_id_type=MESH)

    for i in range(bits):
        pl.semaphore_signal(
            barrier, inc=1, device_id={"dp": partner(0, i)[0]}, device_id_type=MESH
        )

    load_t.wait()
    load_q.start()
    load_o.start()
    for h in range(2):
        load_g(h).start()

    strip = rows // pieces

    def lines(p):
        return pl.ds(pl.multiple_of(p * strip, 16), strip)

    def norm(p):
        def one(r, carry):
            at = pl.multiple_of(p * strip + r * NORM_ROWS, NORM_ROWS)
            here = pl.ds(at, NORM_ROWS)
            values = tok[here, :].astype(f32)
            center = jnp.mean(values, axis=-1, keepdims=True)
            values = values - center
            spread = jnp.mean(values * values, axis=-1, keepdims=True)
            scaled = values * lax.rsqrt(spread + 1e-06) * gain[...] + bias[...]
            blocks[me, here, :] = scaled.astype(bf16)
            return carry

        lax.fori_loop(0, strip // NORM_ROWS, one, 0)

    def own(slot, h, p):
        at = blocks.at[slot, lines(p), side(h)]
        return remote(at, at, own_send.at[p], own_recv.at[p], mate)

    def rest(slot, h):
        at = blocks.at[slot, :, side(h)]
        return remote(at, at, own_send.at[pieces], own_recv.at[pieces], mate)

    def raw(h):
        return remote(
            tok.at[:, side(h)], tok_mate, own_send.at[pieces + 1], own_recv.at[pieces + 1], mate
        )

    def hop_up(slot, j, p):
        at = blocks.at[slot, lines(p), side(s)]
        return remote(at, at, up_send.at[j], up_recv.at[j, p], above)

    def hop_dn(slot, j, p):
        at = blocks.at[slot, lines(p), side(s)]
        return remote(at, at, dn_send.at[j], dn_recv.at[j, p], below)

    def add_up(slot, j, p):
        return remote(
            theirs.at[slot, :, sub(p)],
            chain.at[chain_up(c + 1, j), :, sub(p)],
            up_send.at[j],
            up_recv.at[j, p],
            above,
        )

    def add_dn(slot, j, p):
        return remote(
            theirs.at[slot, :, sub(p)],
            chain.at[chain_dn(c - 1, j), :, sub(p)],
            dn_send.at[j],
            dn_recv.at[j, p],
            below,
        )

    def to_mate(slot, p):
        at = blocks.at[slot, lines(p), side(s)]
        return remote(at, at, mx_send.at[slot], mx_recv.at[slot], mate)

    def from_mate(slot):
        at = blocks.at[slot, :, side(1 - s)]
        return remote(at, at, mx_send.at[slot], mx_recv.at[slot], mate)

    def share(k, slot):
        return remote(stage.at[k], theirs.at[slot], mp_send.at[k], mp_recv.at[slot], mate)

    def first_hops(p):
        @pl.when(up > 0)
        def _():
            hop_up(2 * c, 0, p).start()

        @pl.when(dn > 0)
        def _():
            hop_dn(2 * c, 0, p).start()

    norm(0)
    pl.semaphore_wait(barrier, 1 + up + dn + bits)
    for h in range(2):
        scatter(h, 0).start()

    def opening(p, carry):
        @pl.when(p > 0)
        def _():
            norm(p)

        own(me, 1 - s, p).start()

        @pl.when(s == 0)
        def _():
            first_hops(p)

        return carry

    lax.fori_loop(0, pieces, opening, 0)
    rest(me, s).start()
    raw(1 - s).start()

    def opening_mate(p, carry):
        own(mate, s, p).wait_recv()

        @pl.when(s == 1)
        def _():
            first_hops(p)

        return carry

    lax.fori_loop(0, pieces, opening_mate, 0)

    @pl.when(dn == 0)
    def _():
        chain[chain_up(c, 2 * c), :, :] = jnp.zeros((rows, half), bf16)
        chain[chain_up(c, slots - 1), :, :] = jnp.zeros((rows, half), bf16)

    @pl.when(up == 0)
    def _():
        chain[chain_dn(c, 2 * high), :, :] = jnp.zeros((rows, half), bf16)
        chain[chain_dn(c, slots - 1), :, :] = jnp.zeros((rows, half), bf16)

    rest(mate, 1 - s).wait_recv()
    raw(s).wait_recv()
    for p in range(pieces):
        own(me, 1 - s, p).wait_send()
    rest(me, s).wait_send()
    raw(1 - s).wait_send()
    load_q.wait()
    load_o.wait()

    def project(slot):
        def one(which, carry):
            qkv[which, :, :] = jnp.dot(
                blocks[slot], wq[which], preferred_element_type=f32
            ).astype(bf16)
            return carry

        lax.fori_loop(0, 3, one, 0)

    def attend():
        for image in range(rows // SEQ):
            here = slice(image * SEQ, (image + 1) * SEQ)
            for h in range(inner // HEAD):
                lanes = slice(h * HEAD, (h + 1) * HEAD)
                scores = lax.dot_general(
                    qkv[0, here, lanes],
                    qkv[1, here, lanes],
                    (((1,), (1,)), ((), ())),
                    preferred_element_type=f32,
                ) * HEAD ** (-0.5)
                expsc = jnp.exp(scores - jnp.max(scores, axis=-1, keepdims=True))
                attn = (expsc / jnp.sum(expsc, axis=-1, keepdims=True)).astype(bf16)
                ctx[here, lanes] = jnp.dot(
                    attn, qkv[2, here, lanes], preferred_element_type=f32
                ).astype(bf16)

    block = half // 2

    def output(slot, k):
        for i in range(2):
            at = pl.ds(pl.multiple_of((1 - s) * half + i * block, 128), block)
            stage[k, :, i * block : (i + 1) * block] = jnp.dot(
                ctx[...], wo[:, at], preferred_element_type=f32
            ).astype(bf16)
        share(k, slot).start()
        for i in range(2):
            at = pl.ds(pl.multiple_of(s * half + i * block, 128), block)
            to = pl.ds(pl.multiple_of((1 - s) * half + i * block, 128), block)
            blocks[slot, :, to] = jnp.dot(
                ctx[...], wo[:, at], preferred_element_type=f32
            ).astype(bf16)

    def mine(slot, p):
        return blocks[slot, :, cols(1 - s, p)].astype(f32) + theirs[slot, :, sub(p)].astype(f32)

    def finish(slot, p, foreign):
        value = (
            mine(slot, p)
            + chain[chain_up(c, jnp.where(slot % 2 == 0, 2 * c, slots - 1)), :, sub(p)].astype(f32)
            + chain[chain_dn(c, jnp.where(slot % 2 == 0, 2 * high, slots - 1)), :, sub(p)].astype(f32)
        )
        if foreign:
            fin[:, sub(p)] = (tok_mate[:, sub(p)].astype(f32) + value).astype(bf16)
            give(p).start()
        else:
            out[:, cols(s, p)] = (tok[:, cols(s, p)].astype(f32) + value).astype(bf16)

    def give(p):
        return remote(fin.at[:, sub(p)], out.at[:, cols(s, p)], fin_send.at[p], fin_recv.at[p], mate)

    def take(p):
        return remote(fin.at[:, sub(p)], out.at[:, cols(1 - s, p)], fin_send.at[p], fin_recv.at[p], mate)

    top = 1 - up

    def candidate(j, k):
        a = j - 1
        has_above = jnp.minimum(jnp.maximum(2 * high - a, 0), 1)
        has_below = jnp.minimum(jnp.maximum(2 * c - a, 0), 1)
        from_above = jnp.where(k == 0, 1 - top, 0)
        from_below = jnp.where(k == 0, top, 1 - top)
        later = from_above * has_above + from_below * has_below
        exists = jnp.where(j == 0, 1, later)
        slot = jnp.where(from_above == 1, gather_above(a), gather_below(a))
        return exists, jnp.where(j == 0, 2 * c + k, slot)

    def tick(j, p):
        k = p // 2
        exists, slot = candidate(j, k)
        active = jnp.where(p < 4, exists, 0)

        @pl.when(active * (1 - p % 2) > 0)
        def _():
            @pl.when(j > 0)
            def _():
                from_mate(slot).wait_recv()

            project(slot)

        @pl.when(active * (p % 2) > 0)
        def _():
            attend()
            output(slot, k)

        last = jnp.where(j == slots - 1, 1, 0)

        @pl.when(last * jnp.where(p == 0, 1, 0) > 0)
        def _():
            share(0, 2 * c).wait_recv()
            share(0, 2 * c + 1).wait_recv()
            for ab in range(2):
                @pl.when(s == ab)
                def _():
                    def one(q, carry):
                        finish(2 * c, q, ab == 1)
                        return carry

                    lax.fori_loop(0, pieces, one, 0)

        @pl.when(dn > 0)
        def _():
            @pl.when(j < 2 * c)
            def _():
                image = gather_below(j)
                hop_up(image, j, p).wait_recv()

                @pl.when(up > 0)
                def _():
                    hop_up(image, j + 1, p).start()

                to_mate(image, p).start()

            @pl.when(j >= 2 * c)
            def _():
                image = sum_into_up(c, j)
                at = chain_up(c, j)
                remote(
                    theirs.at[image, :, sub(p)],
                    chain.at[at, :, sub(p)],
                    up_send.at[j],
                    up_recv.at[j, p],
                    above,
                ).wait_recv()

                @pl.when(image >= 2 * c + 2)
                def _():
                    @pl.when(p == 0)
                    def _():
                        share(0, image).wait_recv()

                    theirs[image, :, sub(p)] = (
                        mine(image, p) + chain[at, :, sub(p)].astype(f32)
                    ).astype(bf16)
                    add_up(image, j + 1, p).start()

        @pl.when(up > 0)
        def _():
            @pl.when(j < 2 * high)
            def _():
                image = gather_above(j)
                hop_dn(image, j, p).wait_recv()

                @pl.when(dn > 0)
                def _():
                    hop_dn(image, j + 1, p).start()

                to_mate(image, p).start()

            @pl.when(j >= 2 * high)
            def _():
                image = sum_into_dn(c, j)
                at = chain_dn(c, j)
                remote(
                    theirs.at[image, :, sub(p)],
                    chain.at[at, :, sub(p)],
                    dn_send.at[j],
                    dn_recv.at[j, p],
                    below,
                ).wait_recv()

                @pl.when(image < 2 * c)
                def _():
                    @pl.when(p == 0)
                    def _():
                        share(0, image).wait_recv()

                    theirs[image, :, sub(p)] = (
                        mine(image, p) + chain[at, :, sub(p)].astype(f32)
                    ).astype(bf16)
                    add_dn(image, j + 1, p).start()

        @pl.when(up * jnp.where(p == 0, 1, 0) * jnp.where(j == 2 * c, 1, 0) > 0)
        def _():
            for q in range(pieces):
                hop_up(2 * c + 1, 2 * c + 1, q).start()

        @pl.when(dn * jnp.where(p == 0, 1, 0) * jnp.where(j == 2 * high, 1, 0) > 0)
        def _():
            for q in range(pieces):
                hop_dn(2 * c + 1, 2 * high + 1, q).start()

        begin = jnp.where(p == 3, 1, 0) * jnp.minimum(j, 1) * (1 - last)

        @pl.when(begin * (1 - dn) * up > 0)
        def _():
            image = sum_into_up(c + 1, j + 1)
            share(0, image).wait_recv()

            def one(q, carry):
                theirs[image, :, sub(q)] = mine(image, q).astype(bf16)
                add_up(image, j + 1, q).start()
                return carry

            lax.fori_loop(0, pieces, one, 0)

        @pl.when(begin * (1 - up) * dn > 0)
        def _():
            image = sum_into_dn(c - 1, j + 1)
            share(0, image).wait_recv()

            def one(q, carry):
                theirs[image, :, sub(q)] = mine(image, q).astype(bf16)
                add_dn(image, j + 1, q).start()
                return carry

            lax.fori_loop(0, pieces, one, 0)

        for ab in range(2):
            @pl.when(last * jnp.where(s == ab, 1, 0) > 0)
            def _():
                finish(2 * c + 1, p, ab == 0)

        for e, when in enumerate(times):
            @pl.when(j * pieces + p == when)
            def _():
                grad_event(e)

        @pl.when(p == pieces - 1)
        def _():
            for b in range(2):
                there, image = candidate(j, b)

                @pl.when(there > 0)
                def _():
                    share(b, image).wait_send()

    def slot_loop(j, carry):
        def piece_loop(p, inside):
            tick(j, p)
            return inside

        return lax.fori_loop(0, pieces, piece_loop, carry)

    lax.fori_loop(0, slots, slot_loop, 0)

    for p in range(pieces):
        take(p).wait_recv()

    def drain(j, carry):
        @pl.when(up > 0)
        def _():
            remote(
                blocks.at[0, :, side(s)], blocks.at[0, :, side(s)], up_send.at[j], up_recv.at[0, 0], above
            ).wait_send()

        @pl.when(dn > 0)
        def _():
            remote(
                blocks.at[0, :, side(s)], blocks.at[0, :, side(s)], dn_send.at[j], dn_recv.at[0, 0], below
            ).wait_send()

        @pl.when(j // 2 != c)
        def _():
            from_mate(j).wait_send()

        return carry

    lax.fori_loop(0, slots, drain, 0)
    for p in range(pieces):
        give(p).wait_send()
    for h in range(2):
        for i in range(bits):
            scatter(h, i).wait_send()
            collect(h, i).wait_send()


def spread(mixed, total, mixed_hbm, total_hbm, wide, sem):
    parts = wide.shape[0]
    rows = wide.shape[1]
    first = pltpu.make_async_copy(mixed, mixed_hbm, sem.at[parts])
    first.start()

    def put(i):
        at = pl.ds(pl.multiple_of(i * rows, 8), rows)
        return pltpu.make_async_copy(wide.at[i], total_hbm.at[at, :], sem.at[i])

    def one(i, carry):
        at = pl.ds(pl.multiple_of(i * rows, 8), rows)
        wide[i, :, :] = total[at, :].astype(jnp.float32)
        put(i).start()
        return carry

    lax.fori_loop(0, parts, one, 0)

    def done(i, carry):
        put(i).wait()
        return carry

    lax.fori_loop(0, parts, done, 0)
    first.wait()


def body(n, groups, tokens, ln_gain, ln_bias, w_qkv, w_out, grad_partial):
    local_rows = tokens[0]
    rows, width = local_rows.shape
    inner = w_out.shape[0]
    grows = grad_partial.shape[1]
    chips = n // 2
    slots = 2 * chips
    bits = groups.bit_length() - 1
    half = width // 2
    pieces = pieces_of(half)
    dma = pltpu.SemaphoreType.DMA
    flops = 2 * rows * n * width * inner * 4
    vmem = pl.BlockSpec(memory_space=pltpu.VMEM)
    hbm = pl.BlockSpec(memory_space=pl.ANY)
    bf16 = jnp.bfloat16
    results = (rows + grows) * width * 2
    income = sum(grows >> (i + 2) for i in range(bits))
    mixed, total = pl.pallas_call(
        functools.partial(kernel, n, groups),
        out_shape=(pltpu.VMEM((rows, width), bf16), pltpu.VMEM((grows, width), bf16)),
        in_specs=[hbm, vmem, vmem, hbm, hbm, hbm],
        out_specs=(vmem, vmem),
        scratch_shapes=[
            pltpu.VMEM((3, width, inner), bf16),
            pltpu.VMEM((inner, width), bf16),
            pltpu.VMEM((rows, width), bf16),
            pltpu.VMEM((rows, half), bf16),
            pltpu.VMEM((n, rows, width), bf16),
            pltpu.VMEM((n, rows, half), bf16),
            pltpu.VMEM((2, rows, half), bf16),
            pltpu.VMEM((slots + 2, rows, half), bf16),
            pltpu.VMEM((rows, half), bf16),
            pltpu.VMEM((3, rows, inner), bf16),
            pltpu.VMEM((rows, inner), bf16),
            pltpu.VMEM((2, income, width), bf16),
            dma((5,)),
            dma((pieces + 2,)),
            dma((pieces + 2,)),
            dma((slots,)),
            dma((slots, pieces)),
            dma((slots,)),
            dma((slots, pieces)),
            dma((n,)),
            dma((n,)),
            dma((2,)),
            dma((n,)),
            dma((pieces,)),
            dma((pieces,)),
            dma((2, bits)),
            dma((2, bits)),
            dma((2, bits)),
            dma((2, bits)),
        ],
        compiler_params=pltpu.CompilerParams(
            collective_id=0, has_side_effects=True, vmem_limit_bytes=66_900_000 - results
        ),
        cost_estimate=pl.CostEstimate(
            flops=flops * 8, bytes_accessed=300_000_000, transcendentals=0
        ),
    )(
        local_rows,
        ln_gain.reshape(1, width),
        ln_bias.reshape(1, width),
        jnp.transpose(w_qkv, (1, 0, 2)),
        w_out,
        grad_partial[0],
    )
    parts = grows // 16
    mixed, grad_sum = pl.pallas_call(
        spread,
        out_shape=(
            jax.ShapeDtypeStruct((rows, width), bf16),
            jax.ShapeDtypeStruct((grows, width), jnp.float32),
        ),
        in_specs=[vmem, vmem],
        out_specs=(hbm, hbm),
        scratch_shapes=[
            pltpu.VMEM((parts, grows // parts, width), jnp.float32),
            dma((parts + 1,)),
        ],
        compiler_params=pltpu.CompilerParams(vmem_limit_bytes=grows * width * 4 + 2_000_000),
        cost_estimate=pl.CostEstimate(
            flops=grows * width, bytes_accessed=grows * width * 6, transcendentals=0
        ),
    )(mixed, total)
    return (mixed[None], grad_sum)


def solution(mesh):
    placed = (
        P("dp", "mp", None),
        P(),
        P(),
        P(None, None, "mp"),
        P("mp", None),
        P("dp", "mp", None),
    )
    return jax.shard_map(
        functools.partial(body, mesh.shape["mp"], mesh.shape["dp"]),
        mesh=mesh,
        in_specs=placed,
        out_specs=(P("dp", "mp", None), P("mp", None)),
        check_vma=False,
    )
```

```python
import functools

import jax
import jax.numpy as jnp
from jax import lax
from jax.experimental import pallas as pl
from jax.experimental.pallas import tpu as pltpu
from jax.sharding import PartitionSpec as P

HEAD = 128
SEQ = 128
NORM_ROWS = 16
MESH = pl.DeviceIdType.MESH


def pieces_of(half):
    return next(p for p in (4, 5) if half % (p * 128) == 0)


def kernel(
    n,
    groups,
    tok_hbm,
    gain,
    bias,
    wq_hbm,
    wo_hbm,
    grad_hbm,
    out,
    total,
    wq,
    wo,
    tok,
    blocks,
    theirs,
    stage,
    chain,
    cross,
    other,
    qkv,
    ctx,
    income,
    load_sem,
    own_send,
    own_recv,
    up_send,
    up_recv,
    dn_send,
    dn_recv,
    mx_send,
    mx_recv,
    mp_send,
    mp_recv,
    ot_send,
    ot_recv,
    xu_recv,
    xd_recv,
    rs_send,
    rs_recv,
    ag_send,
    ag_recv,
):
    bits = groups.bit_length() - 1
    assert groups == 1 << bits
    group = lax.axis_index("dp")
    chips = n // 2
    slots = 2 * chips
    me = lax.axis_index("mp")
    c = me // 2
    s = me % 2
    mate = c * 2 + 1 - s
    above = me + 2
    below = me - 2
    high = chips - 1 - c
    up = jnp.minimum(high, 1)
    dn = jnp.minimum(c, 1)
    rows, width = tok.shape
    half = width // 2
    pieces = pieces_of(half)
    wide = half // pieces
    inner = wo.shape[0]
    f32 = jnp.float32
    bf16 = jnp.bfloat16

    def remote(src, dst, send, recv, target):
        return pltpu.make_async_remote_copy(
            src_ref=src,
            dst_ref=dst,
            send_sem=send,
            recv_sem=recv,
            device_id={"mp": target},
            device_id_type=MESH,
        )

    def side(h):
        return pl.ds(pl.multiple_of(h * half, 128), half)

    def cols(h, p):
        return pl.ds(pl.multiple_of(h * half + p * wide, 128), wide)

    def sub(p):
        return pl.ds(pl.multiple_of(p * wide, 128), wide)

    def gather_above(a):
        first = a < high
        return jnp.where(first, 2 * (c + 1 + a), 2 * (c + 2 * high - a) + 1)

    def gather_below(a):
        first = a < c
        return jnp.where(first, 2 * (c - 1 - a), 2 * (a - c) + 1)

    def sum_into_up(chip, j):
        first = j < chips + chip
        return jnp.where(first, 2 * (j - chip), 2 * (chip - 1 + slots - j) + 1)

    def sum_into_dn(chip, j):
        mirror = chips - 1 - chip
        first = j < chips + mirror
        t = jnp.where(first, j - mirror, mirror - 1 + slots - j)
        return 2 * (chips - 1 - t) + jnp.where(first, 0, 1)

    def chain_up(chip, j):
        return j - 2 * chip

    def chain_dn(chip, j):
        return 2 * (chips - chip) + j - 2 * (chips - 1 - chip)

    load_t = pltpu.make_async_copy(tok_hbm, tok, load_sem.at[0])
    load_q = pltpu.make_async_copy(wq_hbm, wq, load_sem.at[1])
    load_o = pltpu.make_async_copy(wo_hbm, wo, load_sem.at[2])
    load_t.start()

    grows = grad_hbm.shape[0] // 2

    def partner(h, i):
        bit = 1 << (i if h == 0 else bits - 1 - i)
        side_of = (group // bit) % 2
        return group + bit * (1 - 2 * side_of), side_of

    def region(h, i):
        base = h * grows
        size = grows
        for step in range(i + 1):
            size = size // 2
            if step < i:
                base = base + partner(h, step)[1] * size
        keep = partner(h, i)[1]
        return base + keep * size, base + (1 - keep) * size, size

    offset = [0]
    for step in range(bits):
        offset.append(offset[-1] + (grows >> (step + 1)))

    def span(base, size):
        return pl.ds(pl.multiple_of(base, 16), size)

    def scatter(h, i):
        _, away, size = region(h, i)
        if i == 0:
            source = grad_hbm.at[span(away, size), :]
        else:
            source = income.at[h, span(offset[i - 1] + away - region(h, i - 1)[0], size), :]
        return pltpu.make_async_remote_copy(
            src_ref=source,
            dst_ref=income.at[h, offset[i] : offset[i] + size, :],
            send_sem=rs_send.at[h, i],
            recv_sem=rs_recv.at[h, i],
            device_id={"dp": partner(h, i)[0]},
            device_id_type=MESH,
        )

    def collect(h, i):
        keep, _, size = region(h, i)
        at = total.at[span(keep, size), :]
        return pltpu.make_async_remote_copy(
            src_ref=at,
            dst_ref=at,
            send_sem=ag_send.at[h, i],
            recv_sem=ag_recv.at[h, i],
            device_id={"dp": partner(h, i)[0]},
            device_id_type=MESH,
        )

    def collected(h, i):
        _, away, size = region(h, i)
        at = total.at[span(away, size), :]
        return pltpu.make_async_remote_copy(
            src_ref=at,
            dst_ref=at,
            send_sem=ag_send.at[h, i],
            recv_sem=ag_recv.at[h, i],
            device_id={"dp": partner(h, i)[0]},
            device_id_type=MESH,
        )

    def load_g(h):
        keep, _, size = region(h, 0)
        return pltpu.make_async_copy(
            grad_hbm.at[span(keep, size), :], total.at[span(keep, size), :], load_sem.at[3 + h]
        )

    def grad_event(e):
        for h in range(2):
            if e < bits:
                if e == 0:
                    load_g(h).wait()
                scatter(h, e).wait_recv()
                keep, _, size = region(h, e)

                def add(base, count, leaves):
                    def one(r, carry):
                        here = span(base + r * 16, 16)
                        there = span(offset[e] + base - keep + r * 16, 16)
                        both = total[here, :].astype(f32) + income[h, there, :].astype(f32)
                        if leaves:
                            income[h, there, :] = both.astype(bf16)
                        else:
                            total[here, :] = both.astype(bf16)
                        return carry

                    lax.fori_loop(0, count // 16, one, 0)

                if e + 1 < bits:
                    stay, leave, count = region(h, e + 1)
                    add(leave, count, True)
                    scatter(h, e + 1).start()
                    add(stay, count, False)
                else:
                    add(keep, size, False)
                    collect(h, e).start()
            else:
                i = 2 * bits - 1 - e
                collected(h, i).wait_recv()
                if i > 0:
                    collect(h, i - 1).start()


    times = []
    at_tick = 0
    for e in range(2 * bits):
        step = e if e < bits else 2 * bits - 1 - e
        lines = (grows >> (step + 1)) * width
        at_tick += -(-lines // (rows * wide)) + 1
        times.append(min(at_tick, slots * pieces - 2 * bits + e))

    barrier = pltpu.get_barrier_semaphore()
    pl.semaphore_signal(barrier, inc=1, device_id={"mp": mate}, device_id_type=MESH)

    @pl.when(up > 0)
    def _():
        for core in range(2):
            target = 2 * (c + 1) + core
            pl.semaphore_signal(barrier, inc=1, device_id={"mp": target}, device_id_type=MESH)

    @pl.when(dn > 0)
    def _():
        for core in range(2):
            target = 2 * (c - 1) + core
            pl.semaphore_signal(barrier, inc=1, device_id={"mp": target}, device_id_type=MESH)

    for i in range(bits):
        pl.semaphore_signal(
            barrier, inc=1, device_id={"dp": partner(0, i)[0]}, device_id_type=MESH
        )

    load_t.wait()
    load_q.start()
    load_o.start()
    for h in range(2):
        load_g(h).start()

    strip = rows // pieces

    def lines(p):
        return pl.ds(pl.multiple_of(p * strip, 16), strip)

    def norm(p):
        def one(r, carry):
            at = pl.multiple_of(p * strip + r * NORM_ROWS, NORM_ROWS)
            here = pl.ds(at, NORM_ROWS)
            values = tok[here, :].astype(f32)
            center = jnp.mean(values, axis=-1, keepdims=True)
            values = values - center
            spread = jnp.mean(values * values, axis=-1, keepdims=True)
            scaled = values * lax.rsqrt(spread + 1e-06) * gain[...] + bias[...]
            blocks[me, here, :] = scaled.astype(bf16)
            return carry

        lax.fori_loop(0, strip // NORM_ROWS, one, 0)

    def own(slot, h, p):
        at = blocks.at[slot, lines(p), side(h)]
        return remote(at, at, own_send.at[p], own_recv.at[p], mate)

    def rest(slot, h):
        at = blocks.at[slot, :, side(h)]
        return remote(at, at, own_send.at[pieces], own_recv.at[pieces], mate)

    def hop_up(slot, j, p):
        at = blocks.at[slot, lines(p), side(s)]
        return remote(at, at, up_send.at[j], up_recv.at[j, p], above)

    def hop_dn(slot, j, p):
        at = blocks.at[slot, lines(p), side(s)]
        return remote(at, at, dn_send.at[j], dn_recv.at[j, p], below)

    def add_up(slot, j, p):
        return remote(
            theirs.at[slot, :, sub(p)],
            chain.at[chain_up(c + 1, j), :, sub(p)],
            up_send.at[j],
            up_recv.at[j, p],
            above,
        )

    def add_dn(slot, j, p):
        return remote(
            theirs.at[slot, :, sub(p)],
            chain.at[chain_dn(c - 1, j), :, sub(p)],
            dn_send.at[j],
            dn_recv.at[j, p],
            below,
        )

    def add_cross_up(slot, j, p):
        return remote(
            theirs.at[slot, :, sub(p)],
            cross.at[0, :, sub(p)],
            up_send.at[j],
            xu_recv.at[p],
            2 * (c + 1) + 1 - s,
        )

    def add_cross_dn(slot, j, p):
        return remote(
            theirs.at[slot, :, sub(p)],
            cross.at[1, :, sub(p)],
            dn_send.at[j],
            xd_recv.at[p],
            2 * (c - 1) + 1 - s,
        )

    def pass_up(slot, j, p):
        turn = jnp.where(slot == 2 * (c + 1) + 1 - s, 1, 0)

        @pl.when(turn == 1)
        def _():
            add_cross_up(slot, j, p).start()

        @pl.when(turn == 0)
        def _():
            add_up(slot, j, p).start()

    def pass_dn(slot, j, p):
        turn = jnp.where(slot == 2 * (c - 1) + 1 - s, 1, 0)

        @pl.when(turn == 1)
        def _():
            add_cross_dn(slot, j, p).start()

        @pl.when(turn == 0)
        def _():
            add_dn(slot, j, p).start()

    def reveal():
        return remote(theirs.at[mate], other, ot_send.at[0], ot_recv.at[0], mate)

    def to_mate(slot, p):
        at = blocks.at[slot, lines(p), side(s)]
        return remote(at, at, mx_send.at[slot], mx_recv.at[slot], mate)

    def from_mate(slot):
        at = blocks.at[slot, :, side(1 - s)]
        return remote(at, at, mx_send.at[slot], mx_recv.at[slot], mate)

    def share(k, slot):
        return remote(stage.at[k], theirs.at[slot], mp_send.at[k], mp_recv.at[slot], mate)

    def first_hops(p):
        @pl.when(up > 0)
        def _():
            hop_up(2 * c, 0, p).start()

        @pl.when(dn > 0)
        def _():
            hop_dn(2 * c, 0, p).start()

    norm(0)
    pl.semaphore_wait(barrier, 1 + 2 * up + 2 * dn + bits)
    for h in range(2):
        scatter(h, 0).start()

    def opening(p, carry):
        @pl.when(p > 0)
        def _():
            norm(p)

        own(me, 1 - s, p).start()

        @pl.when(s == 0)
        def _():
            first_hops(p)

        return carry

    lax.fori_loop(0, pieces, opening, 0)
    rest(me, s).start()

    def opening_mate(p, carry):
        own(mate, s, p).wait_recv()

        @pl.when(s == 1)
        def _():
            first_hops(p)

        return carry

    lax.fori_loop(0, pieces, opening_mate, 0)

    @pl.when(dn == 0)
    def _():
        chain[chain_up(c, 2 * c), :, :] = jnp.zeros((rows, half), bf16)
        chain[chain_up(c, slots - 1), :, :] = jnp.zeros((rows, half), bf16)
        cross[0, :, :] = jnp.zeros((rows, half), bf16)

    @pl.when(up == 0)
    def _():
        chain[chain_dn(c, 2 * high), :, :] = jnp.zeros((rows, half), bf16)
        chain[chain_dn(c, slots - 1), :, :] = jnp.zeros((rows, half), bf16)
        cross[1, :, :] = jnp.zeros((rows, half), bf16)

    rest(mate, 1 - s).wait_recv()
    for p in range(pieces):
        own(me, 1 - s, p).wait_send()
    rest(me, s).wait_send()
    load_q.wait()
    load_o.wait()

    def project(slot):
        def one(which, carry):
            qkv[which, :, :] = jnp.dot(
                blocks[slot], wq[which], preferred_element_type=f32
            ).astype(bf16)
            return carry

        lax.fori_loop(0, 3, one, 0)

    def attend():
        for image in range(rows // SEQ):
            here = slice(image * SEQ, (image + 1) * SEQ)
            for h in range(inner // HEAD):
                lanes = slice(h * HEAD, (h + 1) * HEAD)
                scores = lax.dot_general(
                    qkv[0, here, lanes],
                    qkv[1, here, lanes],
                    (((1,), (1,)), ((), ())),
                    preferred_element_type=f32,
                ) * HEAD ** (-0.5)
                expsc = jnp.exp(scores - jnp.max(scores, axis=-1, keepdims=True))
                attn = (expsc / jnp.sum(expsc, axis=-1, keepdims=True)).astype(bf16)
                ctx[here, lanes] = jnp.dot(
                    attn, qkv[2, here, lanes], preferred_element_type=f32
                ).astype(bf16)

    block = half // 2

    def output(slot, k):
        for i in range(2):
            at = pl.ds(pl.multiple_of((1 - s) * half + i * block, 128), block)
            stage[k, :, i * block : (i + 1) * block] = jnp.dot(
                ctx[...], wo[:, at], preferred_element_type=f32
            ).astype(bf16)
        share(k, slot).start()
        for i in range(2):
            at = pl.ds(pl.multiple_of(s * half + i * block, 128), block)
            to = pl.ds(pl.multiple_of((1 - s) * half + i * block, 128), block)
            blocks[slot, :, to] = jnp.dot(
                ctx[...], wo[:, at], preferred_element_type=f32
            ).astype(bf16)

    def mine(slot, p):
        return blocks[slot, :, cols(1 - s, p)].astype(f32) + theirs[slot, :, sub(p)].astype(f32)

    def finish(p):
        from_dn = chain[chain_up(c, jnp.where(s == 0, 2 * c, slots - 1)), :, sub(p)]
        from_up = chain[chain_dn(c, jnp.where(s == 0, 2 * high, slots - 1)), :, sub(p)]
        value = mine(me, p) + from_dn.astype(f32) + from_up.astype(f32)
        out[:, cols(s, p)] = (tok[:, cols(s, p)].astype(f32) + value).astype(bf16)
        value = (
            other[:, sub(p)].astype(f32)
            + cross[0, :, sub(p)].astype(f32)
            + cross[1, :, sub(p)].astype(f32)
        )
        out[:, cols(1 - s, p)] = (tok[:, cols(1 - s, p)].astype(f32) + value).astype(bf16)

    top = 1 - up

    def candidate(j, k):
        a = j - 1
        has_above = jnp.minimum(jnp.maximum(2 * high - a, 0), 1)
        has_below = jnp.minimum(jnp.maximum(2 * c - a, 0), 1)
        from_above = jnp.where(k == 0, 1 - top, 0)
        from_below = jnp.where(k == 0, top, 1 - top)
        later = from_above * has_above + from_below * has_below
        exists = jnp.where(j == 0, 1, later)
        slot = jnp.where(from_above == 1, gather_above(a), gather_below(a))
        return exists, jnp.where(j == 0, 2 * c + k, slot)

    def tick(j, p):
        k = p // 2
        exists, slot = candidate(j, k)
        active = jnp.where(p < 4, exists, 0)

        @pl.when(active * (1 - p % 2) > 0)
        def _():
            @pl.when(j > 0)
            def _():
                from_mate(slot).wait_recv()

            project(slot)

        @pl.when(active * (p % 2) > 0)
        def _():
            attend()
            output(slot, k)

        last = jnp.where(j == slots - 1, 1, 0)

        @pl.when(jnp.where(j == 1, 1, 0) * jnp.where(p == 0, 1, 0) > 0)
        def _():
            share(0, mate).wait_recv()

            def one(q, carry):
                theirs[mate, :, sub(q)] = mine(mate, q).astype(bf16)
                return carry

            lax.fori_loop(0, pieces, one, 0)
            reveal().start()

        @pl.when(last * jnp.where(p == 0, 1, 0) > 0)
        def _():
            share(0, me).wait_recv()
            reveal().wait_recv()

            @pl.when(s == 0)
            def _():
                def one(q, carry):
                    finish(q)
                    return carry

                lax.fori_loop(0, pieces, one, 0)

        @pl.when(dn > 0)
        def _():
            @pl.when(j < 2 * c)
            def _():
                image = gather_below(j)
                hop_up(image, j, p).wait_recv()

                @pl.when(up > 0)
                def _():
                    hop_up(image, j + 1, p).start()

                to_mate(image, p).start()

            @pl.when(j >= 2 * c)
            def _():
                image = sum_into_up(c, j)
                at = chain_up(c, j)

                @pl.when(image != mate)
                def _():
                    remote(
                        theirs.at[image, :, sub(p)],
                        chain.at[at, :, sub(p)],
                        up_send.at[j],
                        up_recv.at[j, p],
                        above,
                    ).wait_recv()

                @pl.when(image == me)
                def _():
                    add_cross_up(image, j, p).wait_recv()

                @pl.when(image >= 2 * c + 2)
                def _():
                    @pl.when(p == 0)
                    def _():
                        share(0, image).wait_recv()

                    theirs[image, :, sub(p)] = (
                        mine(image, p) + chain[at, :, sub(p)].astype(f32)
                    ).astype(bf16)
                    pass_up(image, j + 1, p)

        @pl.when(up > 0)
        def _():
            @pl.when(j < 2 * high)
            def _():
                image = gather_above(j)
                hop_dn(image, j, p).wait_recv()

                @pl.when(dn > 0)
                def _():
                    hop_dn(image, j + 1, p).start()

                to_mate(image, p).start()

            @pl.when(j >= 2 * high)
            def _():
                image = sum_into_dn(c, j)
                at = chain_dn(c, j)

                @pl.when(image != mate)
                def _():
                    remote(
                        theirs.at[image, :, sub(p)],
                        chain.at[at, :, sub(p)],
                        dn_send.at[j],
                        dn_recv.at[j, p],
                        below,
                    ).wait_recv()

                @pl.when(image == me)
                def _():
                    add_cross_dn(image, j, p).wait_recv()

                @pl.when(image < 2 * c)
                def _():
                    @pl.when(p == 0)
                    def _():
                        share(0, image).wait_recv()

                    theirs[image, :, sub(p)] = (
                        mine(image, p) + chain[at, :, sub(p)].astype(f32)
                    ).astype(bf16)
                    pass_dn(image, j + 1, p)

        @pl.when(up * jnp.where(p == 0, 1, 0) * jnp.where(j == 2 * c, 1, 0) > 0)
        def _():
            for q in range(pieces):
                hop_up(2 * c + 1, 2 * c + 1, q).start()

        @pl.when(dn * jnp.where(p == 0, 1, 0) * jnp.where(j == 2 * high, 1, 0) > 0)
        def _():
            for q in range(pieces):
                hop_dn(2 * c + 1, 2 * high + 1, q).start()

        begin = jnp.where(p == 3, 1, 0) * jnp.minimum(j, 1) * (1 - last)

        @pl.when(begin * (1 - dn) * up > 0)
        def _():
            image = sum_into_up(c + 1, j + 1)
            share(0, image).wait_recv()

            def one(q, carry):
                theirs[image, :, sub(q)] = mine(image, q).astype(bf16)
                pass_up(image, j + 1, q)
                return carry

            lax.fori_loop(0, pieces, one, 0)

        @pl.when(begin * (1 - up) * dn > 0)
        def _():
            image = sum_into_dn(c - 1, j + 1)
            share(0, image).wait_recv()

            def one(q, carry):
                theirs[image, :, sub(q)] = mine(image, q).astype(bf16)
                pass_dn(image, j + 1, q)
                return carry

            lax.fori_loop(0, pieces, one, 0)

        @pl.when(last * s > 0)
        def _():
            finish(p)

        for e, when in enumerate(times):
            @pl.when(j * pieces + p == when)
            def _():
                grad_event(e)

        @pl.when(p == pieces - 1)
        def _():
            for b in range(2):
                there, image = candidate(j, b)

                @pl.when(there > 0)
                def _():
                    share(b, image).wait_send()

    def slot_loop(j, carry):
        def piece_loop(p, inside):
            tick(j, p)
            return inside

        return lax.fori_loop(0, pieces, piece_loop, carry)

    lax.fori_loop(0, slots, slot_loop, 0)

    def drain(j, carry):
        @pl.when(up > 0)
        def _():
            remote(
                blocks.at[0, :, side(s)], blocks.at[0, :, side(s)], up_send.at[j], up_recv.at[0, 0], above
            ).wait_send()

        @pl.when(dn > 0)
        def _():
            remote(
                blocks.at[0, :, side(s)], blocks.at[0, :, side(s)], dn_send.at[j], dn_recv.at[0, 0], below
            ).wait_send()

        @pl.when(j // 2 != c)
        def _():
            from_mate(j).wait_send()

        return carry

    lax.fori_loop(0, slots, drain, 0)
    reveal().wait_send()
    for h in range(2):
        for i in range(bits):
            scatter(h, i).wait_send()
            collect(h, i).wait_send()


def spread(mixed, total, mixed_hbm, total_hbm, wide, sem):
    parts = wide.shape[0]
    rows = wide.shape[1]
    first = pltpu.make_async_copy(mixed, mixed_hbm, sem.at[parts])
    first.start()

    def put(i):
        at = pl.ds(pl.multiple_of(i * rows, 8), rows)
        return pltpu.make_async_copy(wide.at[i], total_hbm.at[at, :], sem.at[i])

    def one(i, carry):
        at = pl.ds(pl.multiple_of(i * rows, 8), rows)
        wide[i, :, :] = total[at, :].astype(jnp.float32)
        put(i).start()
        return carry

    lax.fori_loop(0, parts, one, 0)

    def done(i, carry):
        put(i).wait()
        return carry

    lax.fori_loop(0, parts, done, 0)
    first.wait()


def body(n, groups, tokens, ln_gain, ln_bias, w_qkv, w_out, grad_partial):
    local_rows = tokens[0]
    rows, width = local_rows.shape
    inner = w_out.shape[0]
    grows = grad_partial.shape[1]
    chips = n // 2
    slots = 2 * chips
    bits = groups.bit_length() - 1
    half = width // 2
    pieces = pieces_of(half)
    dma = pltpu.SemaphoreType.DMA
    flops = 2 * rows * n * width * inner * 4
    vmem = pl.BlockSpec(memory_space=pltpu.VMEM)
    hbm = pl.BlockSpec(memory_space=pl.ANY)
    bf16 = jnp.bfloat16
    results = (rows + grows) * width * 2
    income = sum(grows >> (i + 2) for i in range(bits))
    mixed, total = pl.pallas_call(
        functools.partial(kernel, n, groups),
        out_shape=(pltpu.VMEM((rows, width), bf16), pltpu.VMEM((grows, width), bf16)),
        in_specs=[hbm, vmem, vmem, hbm, hbm, hbm],
        out_specs=(vmem, vmem),
        scratch_shapes=[
            pltpu.VMEM((3, width, inner), bf16),
            pltpu.VMEM((inner, width), bf16),
            pltpu.VMEM((rows, width), bf16),
            pltpu.VMEM((n, rows, width), bf16),
            pltpu.VMEM((n, rows, half), bf16),
            pltpu.VMEM((2, rows, half), bf16),
            pltpu.VMEM((slots + 2, rows, half), bf16),
            pltpu.VMEM((2, rows, half), bf16),
            pltpu.VMEM((rows, half), bf16),
            pltpu.VMEM((3, rows, inner), bf16),
            pltpu.VMEM((rows, inner), bf16),
            pltpu.VMEM((2, income, width), bf16),
            dma((5,)),
            dma((pieces + 1,)),
            dma((pieces + 1,)),
            dma((slots,)),
            dma((slots, pieces)),
            dma((slots,)),
            dma((slots, pieces)),
            dma((n,)),
            dma((n,)),
            dma((2,)),
            dma((n,)),
            dma((1,)),
            dma((1,)),
            dma((pieces,)),
            dma((pieces,)),
            dma((2, bits)),
            dma((2, bits)),
            dma((2, bits)),
            dma((2, bits)),
        ],
        compiler_params=pltpu.CompilerParams(
            collective_id=0, has_side_effects=True, vmem_limit_bytes=66_900_000 - results
        ),
        cost_estimate=pl.CostEstimate(
            flops=flops * 8, bytes_accessed=300_000_000, transcendentals=0
        ),
    )(
        local_rows,
        ln_gain.reshape(1, width),
        ln_bias.reshape(1, width),
        jnp.transpose(w_qkv, (1, 0, 2)),
        w_out,
        grad_partial[0],
    )
    parts = grows // 16
    mixed, grad_sum = pl.pallas_call(
        spread,
        out_shape=(
            jax.ShapeDtypeStruct((rows, width), bf16),
            jax.ShapeDtypeStruct((grows, width), jnp.float32),
        ),
        in_specs=[vmem, vmem],
        out_specs=(hbm, hbm),
        scratch_shapes=[
            pltpu.VMEM((parts, grows // parts, width), jnp.float32),
            dma((parts + 1,)),
        ],
        compiler_params=pltpu.CompilerParams(vmem_limit_bytes=grows * width * 4 + 2_000_000),
        cost_estimate=pl.CostEstimate(
            flops=grows * width, bytes_accessed=grows * width * 6, transcendentals=0
        ),
    )(mixed, total)
    return (mixed[None], grad_sum)


def solution(mesh):
    placed = (
        P("dp", "mp", None),
        P(),
        P(),
        P(None, None, "mp"),
        P("mp", None),
        P("dp", "mp", None),
    )
    return jax.shard_map(
        functools.partial(body, mesh.shape["mp"], mesh.shape["dp"]),
        mesh=mesh,
        in_specs=placed,
        out_specs=(P("dp", "mp", None), P("mp", None)),
        check_vma=False,
    )
```

```python
import functools

import jax
import jax.numpy as jnp
from jax import lax
from jax.experimental import pallas as pl
from jax.experimental.pallas import tpu as pltpu
from jax.sharding import PartitionSpec as P

HEAD = 128
SEQ = 128
NORM_ROWS = 16
MESH = pl.DeviceIdType.MESH


def pieces_of(half):
    return next(p for p in (4, 5) if half % (p * 128) == 0)


def kernel(
    n,
    groups,
    tok_hbm,
    gain,
    bias,
    wq_hbm,
    wo_hbm,
    grad_hbm,
    out,
    total,
    wq,
    wo,
    tok,
    blocks,
    theirs,
    stage,
    chain,
    cross,
    other,
    qkv,
    ctx,
    income,
    load_sem,
    own_send,
    own_recv,
    up_send,
    up_recv,
    dn_send,
    dn_recv,
    mx_send,
    mx_recv,
    mp_send,
    mp_recv,
    ot_send,
    ot_recv,
    xu_recv,
    xd_recv,
    rs_send,
    rs_recv,
    ag_send,
    ag_recv,
):
    bits = groups.bit_length() - 1
    assert groups == 1 << bits
    group = lax.axis_index("dp")
    chips = n // 2
    slots = 2 * chips
    me = lax.axis_index("mp")
    c = me // 2
    s = me % 2
    mate = c * 2 + 1 - s
    above = me + 2
    below = me - 2
    high = chips - 1 - c
    up = jnp.minimum(high, 1)
    dn = jnp.minimum(c, 1)
    rows, width = tok.shape
    half = width // 2
    pieces = pieces_of(half)
    wide = half // pieces
    inner = wo.shape[0]
    f32 = jnp.float32
    bf16 = jnp.bfloat16

    barrier = pltpu.get_barrier_semaphore()
    pl.semaphore_signal(barrier, inc=1, device_id={"mp": mate}, device_id_type=MESH)

    @pl.when(up > 0)
    def _():
        for core in range(2):
            target = 2 * (c + 1) + core
            pl.semaphore_signal(barrier, inc=1, device_id={"mp": target}, device_id_type=MESH)

    @pl.when(dn > 0)
    def _():
        for core in range(2):
            target = 2 * (c - 1) + core
            pl.semaphore_signal(barrier, inc=1, device_id={"mp": target}, device_id_type=MESH)

    for i in range(bits):
        pl.semaphore_signal(
            barrier, inc=1, device_id={"dp": group + (1 << i) * (1 - 2 * ((group // (1 << i)) % 2))}, device_id_type=MESH
        )

    def remote(src, dst, send, recv, target):
        return pltpu.make_async_remote_copy(
            src_ref=src,
            dst_ref=dst,
            send_sem=send,
            recv_sem=recv,
            device_id={"mp": target},
            device_id_type=MESH,
        )

    def side(h):
        return pl.ds(pl.multiple_of(h * half, 128), half)

    def cols(h, p):
        return pl.ds(pl.multiple_of(h * half + p * wide, 128), wide)

    def sub(p):
        return pl.ds(pl.multiple_of(p * wide, 128), wide)

    def gather_above(a):
        first = a < high
        return jnp.where(first, 2 * (c + 1 + a), 2 * (c + 2 * high - a) + 1)

    def gather_below(a):
        first = a < c
        return jnp.where(first, 2 * (c - 1 - a), 2 * (a - c) + 1)

    def sum_into_up(chip, j):
        first = j < chips + chip
        return jnp.where(first, 2 * (j - chip), 2 * (chip - 1 + slots - j) + 1)

    def sum_into_dn(chip, j):
        mirror = chips - 1 - chip
        first = j < chips + mirror
        t = jnp.where(first, j - mirror, mirror - 1 + slots - j)
        return 2 * (chips - 1 - t) + jnp.where(first, 0, 1)

    def chain_up(chip, j):
        return j - 2 * chip

    def chain_dn(chip, j):
        return 2 * (chips - chip) + j - 2 * (chips - 1 - chip)

    load_t = pltpu.make_async_copy(tok_hbm, tok, load_sem.at[0])
    load_q = pltpu.make_async_copy(wq_hbm, wq, load_sem.at[1])
    load_o = pltpu.make_async_copy(wo_hbm, wo, load_sem.at[2])
    load_t.start()

    grows = grad_hbm.shape[0] // 2

    def partner(h, i):
        bit = 1 << (i if h == 0 else bits - 1 - i)
        side_of = (group // bit) % 2
        return group + bit * (1 - 2 * side_of), side_of

    def region(h, i):
        base = h * grows
        size = grows
        for step in range(i + 1):
            size = size // 2
            if step < i:
                base = base + partner(h, step)[1] * size
        keep = partner(h, i)[1]
        return base + keep * size, base + (1 - keep) * size, size

    offset = [0]
    for step in range(bits):
        offset.append(offset[-1] + (grows >> (step + 1)))

    def span(base, size):
        return pl.ds(pl.multiple_of(base, 16), size)

    def scatter(h, i):
        _, away, size = region(h, i)
        if i == 0:
            source = grad_hbm.at[span(away, size), :]
        else:
            source = income.at[h, span(offset[i - 1] + away - region(h, i - 1)[0], size), :]
        return pltpu.make_async_remote_copy(
            src_ref=source,
            dst_ref=income.at[h, offset[i] : offset[i] + size, :],
            send_sem=rs_send.at[h, i],
            recv_sem=rs_recv.at[h, i],
            device_id={"dp": partner(h, i)[0]},
            device_id_type=MESH,
        )

    def collect(h, i):
        keep, _, size = region(h, i)
        at = total.at[span(keep, size), :]
        return pltpu.make_async_remote_copy(
            src_ref=at,
            dst_ref=at,
            send_sem=ag_send.at[h, i],
            recv_sem=ag_recv.at[h, i],
            device_id={"dp": partner(h, i)[0]},
            device_id_type=MESH,
        )

    def collected(h, i):
        _, away, size = region(h, i)
        at = total.at[span(away, size), :]
        return pltpu.make_async_remote_copy(
            src_ref=at,
            dst_ref=at,
            send_sem=ag_send.at[h, i],
            recv_sem=ag_recv.at[h, i],
            device_id={"dp": partner(h, i)[0]},
            device_id_type=MESH,
        )

    def load_g(h):
        keep, _, size = region(h, 0)
        return pltpu.make_async_copy(
            grad_hbm.at[span(keep, size), :], total.at[span(keep, size), :], load_sem.at[3 + h]
        )

    def grad_event(e):
        for h in range(2):
            if e < bits:
                if e == 0:
                    load_g(h).wait()
                scatter(h, e).wait_recv()
                keep, _, size = region(h, e)

                def add(base, count, leaves):
                    def one(r, carry):
                        here = span(base + r * 16, 16)
                        there = span(offset[e] + base - keep + r * 16, 16)
                        both = total[here, :].astype(f32) + income[h, there, :].astype(f32)
                        if leaves:
                            income[h, there, :] = both.astype(bf16)
                        else:
                            total[here, :] = both.astype(bf16)
                        return carry

                    lax.fori_loop(0, count // 16, one, 0)

                if e + 1 < bits:
                    stay, leave, count = region(h, e + 1)
                    add(leave, count, True)
                    scatter(h, e + 1).start()
                    add(stay, count, False)
                else:
                    add(keep, size, False)
                    collect(h, e).start()
            else:
                i = 2 * bits - 1 - e
                collected(h, i).wait_recv()
                if i > 0:
                    collect(h, i - 1).start()


    times = []
    at_tick = 0
    for e in range(2 * bits):
        step = e if e < bits else 2 * bits - 1 - e
        lines = (grows >> (step + 1)) * width
        at_tick += -(-lines // (rows * wide)) + 1
        times.append(min(at_tick, slots * pieces - 2 * bits + e))

    load_t.wait()
    load_q.start()
    load_o.start()
    for h in range(2):
        load_g(h).start()

    strip = rows // pieces

    def lines(p):
        return pl.ds(pl.multiple_of(p * strip, 16), strip)

    def norm(p):
        def one(r, carry):
            at = pl.multiple_of(p * strip + r * NORM_ROWS, NORM_ROWS)
            here = pl.ds(at, NORM_ROWS)
            values = tok[here, :].astype(f32)
            center = jnp.mean(values, axis=-1, keepdims=True)
            values = values - center
            spread = jnp.mean(values * values, axis=-1, keepdims=True)
            scaled = values * lax.rsqrt(spread + 1e-06) * gain[...] + bias[...]
            blocks[me, here, :] = scaled.astype(bf16)
            return carry

        lax.fori_loop(0, strip // NORM_ROWS, one, 0)

    def own(slot, h, p):
        at = blocks.at[slot, lines(p), side(h)]
        return remote(at, at, own_send.at[p], own_recv.at[p], mate)

    def rest(slot, h):
        at = blocks.at[slot, :, side(h)]
        return remote(at, at, own_send.at[pieces], own_recv.at[pieces], mate)

    def hop_up(slot, j, p):
        at = blocks.at[slot, lines(p), side(s)]
        return remote(at, at, up_send.at[j], up_recv.at[j, p], above)

    def hop_dn(slot, j, p):
        at = blocks.at[slot, lines(p), side(s)]
        return remote(at, at, dn_send.at[j], dn_recv.at[j, p], below)

    def add_up(slot, j, p):
        return remote(
            theirs.at[slot, :, sub(p)],
            chain.at[chain_up(c + 1, j), :, sub(p)],
            up_send.at[j],
            up_recv.at[j, p],
            above,
        )

    def add_dn(slot, j, p):
        return remote(
            theirs.at[slot, :, sub(p)],
            chain.at[chain_dn(c - 1, j), :, sub(p)],
            dn_send.at[j],
            dn_recv.at[j, p],
            below,
        )

    def add_cross_up(slot, j, p):
        return remote(
            theirs.at[slot, :, sub(p)],
            cross.at[0, :, sub(p)],
            up_send.at[j],
            xu_recv.at[p],
            2 * (c + 1) + 1 - s,
        )

    def add_cross_dn(slot, j, p):
        return remote(
            theirs.at[slot, :, sub(p)],
            cross.at[1, :, sub(p)],
            dn_send.at[j],
            xd_recv.at[p],
            2 * (c - 1) + 1 - s,
        )

    def pass_up(slot, j, p):
        turn = jnp.where(slot == 2 * (c + 1) + 1 - s, 1, 0)

        @pl.when(turn == 1)
        def _():
            add_cross_up(slot, j, p).start()

        @pl.when(turn == 0)
        def _():
            add_up(slot, j, p).start()

    def pass_dn(slot, j, p):
        turn = jnp.where(slot == 2 * (c - 1) + 1 - s, 1, 0)

        @pl.when(turn == 1)
        def _():
            add_cross_dn(slot, j, p).start()

        @pl.when(turn == 0)
        def _():
            add_dn(slot, j, p).start()

    def reveal():
        return remote(theirs.at[mate], other, ot_send.at[0], ot_recv.at[0], mate)

    def to_mate(slot, p):
        at = blocks.at[slot, lines(p), side(s)]
        return remote(at, at, mx_send.at[slot], mx_recv.at[slot], mate)

    def from_mate(slot):
        at = blocks.at[slot, :, side(1 - s)]
        return remote(at, at, mx_send.at[slot], mx_recv.at[slot], mate)

    def share(k, slot):
        return remote(stage.at[k], theirs.at[slot], mp_send.at[k], mp_recv.at[slot], mate)

    def first_hops(p):
        @pl.when(up > 0)
        def _():
            hop_up(2 * c, 0, p).start()

        @pl.when(dn > 0)
        def _():
            hop_dn(2 * c, 0, p).start()

    norm(0)
    pl.semaphore_wait(barrier, 1 + 2 * up + 2 * dn + bits)
    for h in range(2):
        scatter(h, 0).start()

    def opening(p, carry):
        @pl.when(p > 0)
        def _():
            norm(p)

        own(me, 1 - s, p).start()

        @pl.when(s == 0)
        def _():
            first_hops(p)

        @pl.when(s * up * jnp.where(p == 0, 1, 0) > 0)
        def _():
            hop_up(2 * c + 1, 2 * c + 1, 0).start()

        @pl.when(s * dn * jnp.where(p == 0, 1, 0) > 0)
        def _():
            hop_dn(2 * c + 1, 2 * high + 1, 0).start()

        return carry

    lax.fori_loop(0, pieces, opening, 0)
    rest(me, s).start()

    def opening_mate(p, carry):
        own(mate, s, p).wait_recv()

        @pl.when(s == 1)
        def _():
            first_hops(p)

        return carry

    lax.fori_loop(0, pieces, opening_mate, 0)

    @pl.when(dn == 0)
    def _():
        chain[chain_up(c, 2 * c), :, :] = jnp.zeros((rows, half), bf16)
        chain[chain_up(c, slots - 1), :, :] = jnp.zeros((rows, half), bf16)
        cross[0, :, :] = jnp.zeros((rows, half), bf16)

    @pl.when(up == 0)
    def _():
        chain[chain_dn(c, 2 * high), :, :] = jnp.zeros((rows, half), bf16)
        chain[chain_dn(c, slots - 1), :, :] = jnp.zeros((rows, half), bf16)
        cross[1, :, :] = jnp.zeros((rows, half), bf16)

    rest(mate, 1 - s).wait_recv()
    for p in range(pieces):
        own(me, 1 - s, p).wait_send()
    rest(me, s).wait_send()
    load_q.wait()
    load_o.wait()

    def project(slot):
        def one(which, carry):
            qkv[which, :, :] = jnp.dot(
                blocks[slot], wq[which], preferred_element_type=f32
            ).astype(bf16)
            return carry

        lax.fori_loop(0, 3, one, 0)

    def attend():
        for image in range(rows // SEQ):
            here = slice(image * SEQ, (image + 1) * SEQ)
            for h in range(inner // HEAD):
                lanes = slice(h * HEAD, (h + 1) * HEAD)
                scores = lax.dot_general(
                    qkv[0, here, lanes],
                    qkv[1, here, lanes],
                    (((1,), (1,)), ((), ())),
                    preferred_element_type=f32,
                ) * HEAD ** (-0.5)
                expsc = jnp.exp(scores - jnp.max(scores, axis=-1, keepdims=True))
                attn = (expsc / jnp.sum(expsc, axis=-1, keepdims=True)).astype(bf16)
                ctx[here, lanes] = jnp.dot(
                    attn, qkv[2, here, lanes], preferred_element_type=f32
                ).astype(bf16)

    block = half // 2

    def output(slot, k):
        for i in range(2):
            at = pl.ds(pl.multiple_of((1 - s) * half + i * block, 128), block)
            stage[k, :, i * block : (i + 1) * block] = jnp.dot(
                ctx[...], wo[:, at], preferred_element_type=f32
            ).astype(bf16)
        share(k, slot).start()
        for i in range(2):
            at = pl.ds(pl.multiple_of(s * half + i * block, 128), block)
            to = pl.ds(pl.multiple_of((1 - s) * half + i * block, 128), block)
            blocks[slot, :, to] = jnp.dot(
                ctx[...], wo[:, at], preferred_element_type=f32
            ).astype(bf16)

    def mine(slot, p):
        return blocks[slot, :, cols(1 - s, p)].astype(f32) + theirs[slot, :, sub(p)].astype(f32)

    def finish(p):
        from_dn = chain[chain_up(c, jnp.where(s == 0, 2 * c, slots - 1)), :, sub(p)]
        from_up = chain[chain_dn(c, jnp.where(s == 0, 2 * high, slots - 1)), :, sub(p)]
        value = mine(me, p) + from_dn.astype(f32) + from_up.astype(f32)
        out[:, cols(s, p)] = (tok[:, cols(s, p)].astype(f32) + value).astype(bf16)
        value = (
            other[:, sub(p)].astype(f32)
            + cross[0, :, sub(p)].astype(f32)
            + cross[1, :, sub(p)].astype(f32)
        )
        out[:, cols(1 - s, p)] = (tok[:, cols(1 - s, p)].astype(f32) + value).astype(bf16)

    top = 1 - up

    def candidate(j, k):
        a = j - 1
        has_above = jnp.minimum(jnp.maximum(2 * high - a, 0), 1)
        has_below = jnp.minimum(jnp.maximum(2 * c - a, 0), 1)
        from_above = jnp.where(k == 0, 1 - top, 0)
        from_below = jnp.where(k == 0, top, 1 - top)
        later = from_above * has_above + from_below * has_below
        exists = jnp.where(j == 0, 1, later)
        slot = jnp.where(from_above == 1, gather_above(a), gather_below(a))
        return exists, jnp.where(j == 0, 2 * c + k, slot)

    def tick(j, p):
        k = p // 2
        exists, slot = candidate(j, k)
        active = jnp.where(p < 4, exists, 0)

        @pl.when(active * (1 - p % 2) > 0)
        def _():
            @pl.when(j > 0)
            def _():
                from_mate(slot).wait_recv()

            project(slot)

        @pl.when(active * (p % 2) > 0)
        def _():
            attend()
            output(slot, k)

        last = jnp.where(j == slots - 1, 1, 0)

        @pl.when(jnp.where(j == 1, 1, 0) * jnp.where(p == 0, 1, 0) > 0)
        def _():
            share(0, mate).wait_recv()

            def one(q, carry):
                theirs[mate, :, sub(q)] = mine(mate, q).astype(bf16)
                return carry

            lax.fori_loop(0, pieces, one, 0)
            reveal().start()

        @pl.when(last * jnp.where(p == 0, 1, 0) > 0)
        def _():
            share(0, me).wait_recv()
            reveal().wait_recv()

            @pl.when(s == 0)
            def _():
                def one(q, carry):
                    finish(q)
                    return carry

                lax.fori_loop(0, pieces, one, 0)

        begin = jnp.where(p == 2, 1, 0) * jnp.minimum(j, 1) * (1 - last)

        @pl.when(begin * (1 - dn) * up > 0)
        def _():
            image = sum_into_up(c + 1, j + 1)
            share(0, image).wait_recv()

            def one(q, carry):
                theirs[image, :, sub(q)] = mine(image, q).astype(bf16)
                pass_up(image, j + 1, q)
                return carry

            lax.fori_loop(0, pieces, one, 0)

        @pl.when(begin * (1 - up) * dn > 0)
        def _():
            image = sum_into_dn(c - 1, j + 1)
            share(0, image).wait_recv()

            def one(q, carry):
                theirs[image, :, sub(q)] = mine(image, q).astype(bf16)
                pass_dn(image, j + 1, q)
                return carry

            lax.fori_loop(0, pieces, one, 0)

        @pl.when(dn > 0)
        def _():
            @pl.when(j < 2 * c)
            def _():
                image = gather_below(j)
                hop_up(image, j, p).wait_recv()

                @pl.when(up > 0)
                def _():
                    hop_up(image, j + 1, p).start()

                to_mate(image, p).start()

            @pl.when(j >= 2 * c)
            def _():
                image = sum_into_up(c, j)
                at = chain_up(c, j)

                @pl.when(image != mate)
                def _():
                    remote(
                        theirs.at[image, :, sub(p)],
                        chain.at[at, :, sub(p)],
                        up_send.at[j],
                        up_recv.at[j, p],
                        above,
                    ).wait_recv()

                @pl.when(image == me)
                def _():
                    add_cross_up(image, j, p).wait_recv()

                @pl.when(image >= 2 * c + 2)
                def _():
                    @pl.when(p == 0)
                    def _():
                        share(0, image).wait_recv()

                    theirs[image, :, sub(p)] = (
                        mine(image, p) + chain[at, :, sub(p)].astype(f32)
                    ).astype(bf16)
                    pass_up(image, j + 1, p)

        @pl.when(up > 0)
        def _():
            @pl.when(j < 2 * high)
            def _():
                image = gather_above(j)
                hop_dn(image, j, p).wait_recv()

                @pl.when(dn > 0)
                def _():
                    hop_dn(image, j + 1, p).start()

                to_mate(image, p).start()

            @pl.when(j >= 2 * high)
            def _():
                image = sum_into_dn(c, j)
                at = chain_dn(c, j)

                @pl.when(image != mate)
                def _():
                    remote(
                        theirs.at[image, :, sub(p)],
                        chain.at[at, :, sub(p)],
                        dn_send.at[j],
                        dn_recv.at[j, p],
                        below,
                    ).wait_recv()

                @pl.when(image == me)
                def _():
                    add_cross_dn(image, j, p).wait_recv()

                @pl.when(image < 2 * c)
                def _():
                    @pl.when(p == 0)
                    def _():
                        share(0, image).wait_recv()

                    theirs[image, :, sub(p)] = (
                        mine(image, p) + chain[at, :, sub(p)].astype(f32)
                    ).astype(bf16)
                    pass_dn(image, j + 1, p)

        @pl.when(up * jnp.where(p == 0, 1, 0) * jnp.where(j == 2 * c, 1, 0) > 0)
        def _():
            @pl.when(s == 0)
            def _():
                hop_up(2 * c + 1, 2 * c + 1, 0).start()

            for q in range(1, pieces):
                hop_up(2 * c + 1, 2 * c + 1, q).start()

        @pl.when(dn * jnp.where(p == 0, 1, 0) * jnp.where(j == 2 * high, 1, 0) > 0)
        def _():
            @pl.when(s == 0)
            def _():
                hop_dn(2 * c + 1, 2 * high + 1, 0).start()

            for q in range(1, pieces):
                hop_dn(2 * c + 1, 2 * high + 1, q).start()

        @pl.when(last * s > 0)
        def _():
            finish(p)

        for e, when in enumerate(times):
            @pl.when(j * pieces + p == when)
            def _():
                grad_event(e)

        @pl.when(p == pieces - 1)
        def _():
            for b in range(2):
                there, image = candidate(j, b)

                @pl.when(there > 0)
                def _():
                    share(b, image).wait_send()

    def slot_loop(j, carry):
        def piece_loop(p, inside):
            tick(j, p)
            return inside

        return lax.fori_loop(0, pieces, piece_loop, carry)

    lax.fori_loop(0, slots, slot_loop, 0)

    def drain(j, carry):
        @pl.when(up > 0)
        def _():
            remote(
                blocks.at[0, :, side(s)], blocks.at[0, :, side(s)], up_send.at[j], up_recv.at[0, 0], above
            ).wait_send()

        @pl.when(dn > 0)
        def _():
            remote(
                blocks.at[0, :, side(s)], blocks.at[0, :, side(s)], dn_send.at[j], dn_recv.at[0, 0], below
            ).wait_send()

        @pl.when(j // 2 != c)
        def _():
            from_mate(j).wait_send()

        return carry

    lax.fori_loop(0, slots, drain, 0)
    reveal().wait_send()
    for h in range(2):
        for i in range(bits):
            scatter(h, i).wait_send()
            collect(h, i).wait_send()


def spread(mixed, total, mixed_hbm, total_hbm, wide, sem):
    parts = wide.shape[0]
    rows = wide.shape[1]
    first = pltpu.make_async_copy(mixed, mixed_hbm, sem.at[parts])
    first.start()

    def put(i):
        at = pl.ds(pl.multiple_of(i * rows, 8), rows)
        return pltpu.make_async_copy(wide.at[i], total_hbm.at[at, :], sem.at[i])

    def one(i, carry):
        at = pl.ds(pl.multiple_of(i * rows, 8), rows)
        wide[i, :, :] = total[at, :].astype(jnp.float32)
        put(i).start()
        return carry

    lax.fori_loop(0, parts, one, 0)

    def done(i, carry):
        put(i).wait()
        return carry

    lax.fori_loop(0, parts, done, 0)
    first.wait()


def body(n, groups, tokens, ln_gain, ln_bias, w_qkv, w_out, grad_partial):
    local_rows = tokens[0]
    rows, width = local_rows.shape
    inner = w_out.shape[0]
    grows = grad_partial.shape[1]
    chips = n // 2
    slots = 2 * chips
    bits = groups.bit_length() - 1
    half = width // 2
    pieces = pieces_of(half)
    dma = pltpu.SemaphoreType.DMA
    flops = 2 * rows * n * width * inner * 4
    vmem = pl.BlockSpec(memory_space=pltpu.VMEM)
    hbm = pl.BlockSpec(memory_space=pl.ANY)
    bf16 = jnp.bfloat16
    results = (rows + grows) * width * 2
    income = sum(grows >> (i + 2) for i in range(bits))
    mixed, total = pl.pallas_call(
        functools.partial(kernel, n, groups),
        out_shape=(pltpu.VMEM((rows, width), bf16), pltpu.VMEM((grows, width), bf16)),
        in_specs=[hbm, vmem, vmem, hbm, hbm, hbm],
        out_specs=(vmem, vmem),
        scratch_shapes=[
            pltpu.VMEM((3, width, inner), bf16),
            pltpu.VMEM((inner, width), bf16),
            pltpu.VMEM((rows, width), bf16),
            pltpu.VMEM((n, rows, width), bf16),
            pltpu.VMEM((n, rows, half), bf16),
            pltpu.VMEM((2, rows, half), bf16),
            pltpu.VMEM((slots + 2, rows, half), bf16),
            pltpu.VMEM((2, rows, half), bf16),
            pltpu.VMEM((rows, half), bf16),
            pltpu.VMEM((3, rows, inner), bf16),
            pltpu.VMEM((rows, inner), bf16),
            pltpu.VMEM((2, income, width), bf16),
            dma((5,)),
            dma((pieces + 1,)),
            dma((pieces + 1,)),
            dma((slots,)),
            dma((slots, pieces)),
            dma((slots,)),
            dma((slots, pieces)),
            dma((n,)),
            dma((n,)),
            dma((2,)),
            dma((n,)),
            dma((1,)),
            dma((1,)),
            dma((pieces,)),
            dma((pieces,)),
            dma((2, bits)),
            dma((2, bits)),
            dma((2, bits)),
            dma((2, bits)),
        ],
        compiler_params=pltpu.CompilerParams(
            collective_id=0, has_side_effects=True, vmem_limit_bytes=66_900_000 - results
        ),
        cost_estimate=pl.CostEstimate(
            flops=flops * 8, bytes_accessed=300_000_000, transcendentals=0
        ),
    )(
        local_rows,
        ln_gain.reshape(1, width),
        ln_bias.reshape(1, width),
        jnp.transpose(w_qkv, (1, 0, 2)),
        w_out,
        grad_partial[0],
    )
    parts = grows // 16
    mixed, grad_sum = pl.pallas_call(
        spread,
        out_shape=(
            jax.ShapeDtypeStruct((rows, width), bf16),
            jax.ShapeDtypeStruct((grows, width), jnp.float32),
        ),
        in_specs=[vmem, vmem],
        out_specs=(hbm, hbm),
        scratch_shapes=[
            pltpu.VMEM((parts, grows // parts, width), jnp.float32),
            dma((parts + 1,)),
        ],
        compiler_params=pltpu.CompilerParams(vmem_limit_bytes=grows * width * 4 + 2_000_000),
        cost_estimate=pl.CostEstimate(
            flops=grows * width, bytes_accessed=grows * width * 6, transcendentals=0
        ),
    )(mixed, total)
    return (mixed[None], grad_sum)


def solution(mesh):
    placed = (
        P("dp", "mp", None),
        P(),
        P(),
        P(None, None, "mp"),
        P("mp", None),
        P("dp", "mp", None),
    )
    return jax.shard_map(
        functools.partial(body, mesh.shape["mp"], mesh.shape["dp"]),
        mesh=mesh,
        in_specs=placed,
        out_specs=(P("dp", "mp", None), P("mp", None)),
        check_vma=False,
    )
```

```python
import functools

import jax
import jax.numpy as jnp
from jax import lax
from jax.experimental import pallas as pl
from jax.experimental.pallas import tpu as pltpu
from jax.sharding import PartitionSpec as P

HEAD = 128
SEQ = 128
NORM_ROWS = 16
MESH = pl.DeviceIdType.MESH


def pieces_of(half):
    return next(p for p in (4, 5) if half % (p * 128) == 0)


def kernel(
    n,
    groups,
    tok_hbm,
    gain,
    bias,
    wq_hbm,
    wo_hbm,
    grad_hbm,
    out,
    total,
    wq,
    wo,
    tok,
    blocks,
    theirs,
    stage,
    chain,
    cross,
    other,
    qkv,
    ctx,
    income,
    load_sem,
    own_send,
    own_recv,
    up_send,
    up_recv,
    dn_send,
    dn_recv,
    mx_send,
    mx_recv,
    mp_send,
    mp_recv,
    ot_send,
    ot_recv,
    xu_recv,
    xd_recv,
    rs_send,
    rs_recv,
    ag_send,
    ag_recv,
):
    bits = groups.bit_length() - 1
    assert groups == 1 << bits
    group = lax.axis_index("dp")
    chips = n // 2
    slots = 2 * chips
    me = lax.axis_index("mp")
    c = me // 2
    s = me % 2
    mate = c * 2 + 1 - s
    above = me + 2
    below = me - 2
    high = chips - 1 - c
    up = jnp.minimum(high, 1)
    dn = jnp.minimum(c, 1)
    rows, width = tok.shape
    half = width // 2
    pieces = pieces_of(half)
    wide = half // pieces
    inner = wo.shape[0]
    f32 = jnp.float32
    bf16 = jnp.bfloat16

    barrier = pltpu.get_barrier_semaphore()
    pl.semaphore_signal(barrier, inc=1, device_id={"mp": mate}, device_id_type=MESH)

    @pl.when(up > 0)
    def _():
        for core in range(2):
            target = 2 * (c + 1) + core
            pl.semaphore_signal(barrier, inc=1, device_id={"mp": target}, device_id_type=MESH)

    @pl.when(dn > 0)
    def _():
        for core in range(2):
            target = 2 * (c - 1) + core
            pl.semaphore_signal(barrier, inc=1, device_id={"mp": target}, device_id_type=MESH)

    for i in range(bits):
        pl.semaphore_signal(
            barrier, inc=1, device_id={"dp": group + (1 << i) * (1 - 2 * ((group // (1 << i)) % 2))}, device_id_type=MESH
        )

    def remote(src, dst, send, recv, target):
        return pltpu.make_async_remote_copy(
            src_ref=src,
            dst_ref=dst,
            send_sem=send,
            recv_sem=recv,
            device_id={"mp": target},
            device_id_type=MESH,
        )

    def side(h):
        return pl.ds(pl.multiple_of(h * half, 128), half)

    def cols(h, p):
        return pl.ds(pl.multiple_of(h * half + p * wide, 128), wide)

    def sub(p):
        return pl.ds(pl.multiple_of(p * wide, 128), wide)

    def gather_above(a):
        first = a < high
        return jnp.where(first, 2 * (c + 1 + a), 2 * (c + 2 * high - a) + 1)

    def gather_below(a):
        first = a < c
        return jnp.where(first, 2 * (c - 1 - a), 2 * (a - c) + 1)

    def sum_into_up(chip, j):
        first = j < chips + chip
        return jnp.where(first, 2 * (j - chip), 2 * (chip - 1 + slots - j) + 1)

    def sum_into_dn(chip, j):
        mirror = chips - 1 - chip
        first = j < chips + mirror
        t = jnp.where(first, j - mirror, mirror - 1 + slots - j)
        return 2 * (chips - 1 - t) + jnp.where(first, 0, 1)

    def chain_up(chip, j):
        return j - 2 * chip

    def chain_dn(chip, j):
        return 2 * (chips - chip) + j - 2 * (chips - 1 - chip)

    load_t = pltpu.make_async_copy(tok_hbm, tok, load_sem.at[0])
    load_q = pltpu.make_async_copy(wq_hbm, wq, load_sem.at[1])
    load_o = pltpu.make_async_copy(wo_hbm, wo, load_sem.at[2])
    load_t.start()

    grows = grad_hbm.shape[0] // 2

    def partner(h, i):
        bit = 1 << (i if h == 0 else bits - 1 - i)
        side_of = (group // bit) % 2
        return group + bit * (1 - 2 * side_of), side_of

    def region(h, i):
        base = h * grows
        size = grows
        for step in range(i + 1):
            size = size // 2
            if step < i:
                base = base + partner(h, step)[1] * size
        keep = partner(h, i)[1]
        return base + keep * size, base + (1 - keep) * size, size

    offset = [0]
    for step in range(bits):
        offset.append(offset[-1] + (grows >> (step + 1)))

    def span(base, size):
        return pl.ds(pl.multiple_of(base, 16), size)

    def scatter(h, i):
        _, away, size = region(h, i)
        if i == 0:
            source = grad_hbm.at[span(away, size), :]
        else:
            source = income.at[h, span(offset[i - 1] + away - region(h, i - 1)[0], size), :]
        return pltpu.make_async_remote_copy(
            src_ref=source,
            dst_ref=income.at[h, offset[i] : offset[i] + size, :],
            send_sem=rs_send.at[h, i],
            recv_sem=rs_recv.at[h, i],
            device_id={"dp": partner(h, i)[0]},
            device_id_type=MESH,
        )

    def collect(h, i):
        keep, _, size = region(h, i)
        at = total.at[span(keep, size), :]
        return pltpu.make_async_remote_copy(
            src_ref=at,
            dst_ref=at,
            send_sem=ag_send.at[h, i],
            recv_sem=ag_recv.at[h, i],
            device_id={"dp": partner(h, i)[0]},
            device_id_type=MESH,
        )

    def collected(h, i):
        _, away, size = region(h, i)
        at = total.at[span(away, size), :]
        return pltpu.make_async_remote_copy(
            src_ref=at,
            dst_ref=at,
            send_sem=ag_send.at[h, i],
            recv_sem=ag_recv.at[h, i],
            device_id={"dp": partner(h, i)[0]},
            device_id_type=MESH,
        )

    def load_g(h):
        keep, _, size = region(h, 0)
        return pltpu.make_async_copy(
            grad_hbm.at[span(keep, size), :], total.at[span(keep, size), :], load_sem.at[3 + h]
        )

    def grad_event(e):
        for h in range(2):
            if e < bits:
                if e == 0:
                    load_g(h).wait()
                scatter(h, e).wait_recv()
                keep, _, size = region(h, e)

                def add(base, count, leaves):
                    def one(r, carry):
                        here = span(base + r * 16, 16)
                        there = span(offset[e] + base - keep + r * 16, 16)
                        both = total[here, :].astype(f32) + income[h, there, :].astype(f32)
                        if leaves:
                            income[h, there, :] = both.astype(bf16)
                        else:
                            total[here, :] = both.astype(bf16)
                        return carry

                    lax.fori_loop(0, count // 16, one, 0)

                if e + 1 < bits:
                    stay, leave, count = region(h, e + 1)
                    add(leave, count, True)
                    scatter(h, e + 1).start()
                    add(stay, count, False)
                else:
                    add(keep, size, False)
                    collect(h, e).start()
            else:
                i = 2 * bits - 1 - e
                collected(h, i).wait_recv()
                if i > 0:
                    collect(h, i - 1).start()


    times = []
    at_tick = 0
    for e in range(2 * bits):
        step = e if e < bits else 2 * bits - 1 - e
        lines = (grows >> (step + 1)) * width
        at_tick += -(-lines // (rows * wide)) + 1
        times.append(min(at_tick, slots * pieces - 2 * bits + e))

    load_t.wait()
    load_q.start()
    load_o.start()
    for h in range(2):
        load_g(h).start()

    strip = rows // pieces

    def lines(p):
        return pl.ds(pl.multiple_of(p * strip, 16), strip)

    def norm(p):
        def one(r, carry):
            at = pl.multiple_of(p * strip + r * NORM_ROWS, NORM_ROWS)
            here = pl.ds(at, NORM_ROWS)
            values = tok[here, :].astype(f32)
            center = jnp.mean(values, axis=-1, keepdims=True)
            values = values - center
            spread = jnp.mean(values * values, axis=-1, keepdims=True)
            scaled = values * lax.rsqrt(spread + 1e-06) * gain[...] + bias[...]
            blocks[me, here, :] = scaled.astype(bf16)
            return carry

        lax.fori_loop(0, strip // NORM_ROWS, one, 0)

    def own(slot, h, p):
        at = blocks.at[slot, lines(p), side(h)]
        return remote(at, at, own_send.at[p], own_recv.at[p], mate)

    def rest(slot, h):
        at = blocks.at[slot, :, side(h)]
        return remote(at, at, own_send.at[pieces], own_recv.at[pieces], mate)

    def hop_up(slot, j, p):
        at = blocks.at[slot, lines(p), side(s)]
        return remote(at, at, up_send.at[j], up_recv.at[j, p], above)

    def hop_dn(slot, j, p):
        at = blocks.at[slot, lines(p), side(s)]
        return remote(at, at, dn_send.at[j], dn_recv.at[j, p], below)

    def add_up(slot, j, p):
        return remote(
            theirs.at[slot, :, sub(p)],
            chain.at[chain_up(c + 1, j), :, sub(p)],
            up_send.at[j],
            up_recv.at[j, p],
            above,
        )

    def add_dn(slot, j, p):
        return remote(
            theirs.at[slot, :, sub(p)],
            chain.at[chain_dn(c - 1, j), :, sub(p)],
            dn_send.at[j],
            dn_recv.at[j, p],
            below,
        )

    def add_cross_up(slot, j, p):
        return remote(
            theirs.at[slot, :, sub(p)],
            cross.at[0, :, sub(p)],
            up_send.at[j],
            xu_recv.at[p],
            2 * (c + 1) + 1 - s,
        )

    def add_cross_dn(slot, j, p):
        return remote(
            theirs.at[slot, :, sub(p)],
            cross.at[1, :, sub(p)],
            dn_send.at[j],
            xd_recv.at[p],
            2 * (c - 1) + 1 - s,
        )

    def pass_up(slot, j, p):
        turn = jnp.where(slot == 2 * (c + 1) + 1 - s, 1, 0)

        @pl.when(turn == 1)
        def _():
            add_cross_up(slot, j, p).start()

        @pl.when(turn == 0)
        def _():
            add_up(slot, j, p).start()

    def pass_dn(slot, j, p):
        turn = jnp.where(slot == 2 * (c - 1) + 1 - s, 1, 0)

        @pl.when(turn == 1)
        def _():
            add_cross_dn(slot, j, p).start()

        @pl.when(turn == 0)
        def _():
            add_dn(slot, j, p).start()

    def reveal():
        return remote(theirs.at[mate], other, ot_send.at[0], ot_recv.at[0], mate)

    def to_mate(slot, p):
        at = blocks.at[slot, lines(p), side(s)]
        return remote(at, at, mx_send.at[slot], mx_recv.at[slot], mate)

    def from_mate(slot):
        at = blocks.at[slot, :, side(1 - s)]
        return remote(at, at, mx_send.at[slot], mx_recv.at[slot], mate)

    def share(k, slot):
        return remote(stage.at[k], theirs.at[slot], mp_send.at[k], mp_recv.at[slot], mate)

    def first_hops(p):
        @pl.when(up > 0)
        def _():
            hop_up(2 * c, 0, p).start()

        @pl.when(dn > 0)
        def _():
            hop_dn(2 * c, 0, p).start()

    norm(0)
    pl.semaphore_wait(barrier, 1 + 2 * up + 2 * dn + bits)
    for h in range(2):
        scatter(h, 0).start()

    def opening(p, carry):
        @pl.when(p > 0)
        def _():
            norm(p)

        own(me, 1 - s, p).start()

        @pl.when(s == 0)
        def _():
            first_hops(p)

        @pl.when(s * up * jnp.where(p == 0, 1, 0) > 0)
        def _():
            hop_up(2 * c + 1, 2 * c + 1, 0).start()

        @pl.when(s * dn * jnp.where(p == 0, 1, 0) > 0)
        def _():
            hop_dn(2 * c + 1, 2 * high + 1, 0).start()

        return carry

    lax.fori_loop(0, pieces, opening, 0)
    rest(me, s).start()

    def opening_mate(p, carry):
        own(mate, s, p).wait_recv()

        @pl.when(s == 1)
        def _():
            first_hops(p)

        return carry

    lax.fori_loop(0, pieces, opening_mate, 0)

    @pl.when(dn == 0)
    def _():
        chain[chain_up(c, 2 * c), :, :] = jnp.zeros((rows, half), bf16)
        chain[chain_up(c, slots - 1), :, :] = jnp.zeros((rows, half), bf16)
        cross[0, :, :] = jnp.zeros((rows, half), bf16)

    @pl.when(up == 0)
    def _():
        chain[chain_dn(c, 2 * high), :, :] = jnp.zeros((rows, half), bf16)
        chain[chain_dn(c, slots - 1), :, :] = jnp.zeros((rows, half), bf16)
        cross[1, :, :] = jnp.zeros((rows, half), bf16)

    rest(mate, 1 - s).wait_recv()
    for p in range(pieces):
        own(me, 1 - s, p).wait_send()
    rest(me, s).wait_send()
    load_q.wait()
    load_o.wait()

    def project(slot):
        def one(which, carry):
            qkv[which, :, :] = jnp.dot(
                blocks[slot], wq[which], preferred_element_type=f32
            ).astype(bf16)
            return carry

        lax.fori_loop(0, 3, one, 0)

    def attend():
        for image in range(rows // SEQ):
            here = slice(image * SEQ, (image + 1) * SEQ)
            for h in range(inner // HEAD):
                lanes = slice(h * HEAD, (h + 1) * HEAD)
                scores = lax.dot_general(
                    qkv[0, here, lanes],
                    qkv[1, here, lanes],
                    (((1,), (1,)), ((), ())),
                    preferred_element_type=f32,
                ) * HEAD ** (-0.5)
                expsc = jnp.exp(scores - jnp.max(scores, axis=-1, keepdims=True))
                attn = (expsc / jnp.sum(expsc, axis=-1, keepdims=True)).astype(bf16)
                ctx[here, lanes] = jnp.dot(
                    attn, qkv[2, here, lanes], preferred_element_type=f32
                ).astype(bf16)

    block = half // 2

    def output(slot, k):
        for i in range(2):
            at = pl.ds(pl.multiple_of((1 - s) * half + i * block, 128), block)
            stage[k, :, i * block : (i + 1) * block] = jnp.dot(
                ctx[...], wo[:, at], preferred_element_type=f32
            ).astype(bf16)
        share(k, slot).start()
        for i in range(2):
            at = pl.ds(pl.multiple_of(s * half + i * block, 128), block)
            to = pl.ds(pl.multiple_of((1 - s) * half + i * block, 128), block)
            blocks[slot, :, to] = jnp.dot(
                ctx[...], wo[:, at], preferred_element_type=f32
            ).astype(bf16)

    def mine(slot, p):
        return blocks[slot, :, cols(1 - s, p)].astype(f32) + theirs[slot, :, sub(p)].astype(f32)

    def finish(p):
        from_dn = chain[chain_up(c, jnp.where(s == 0, 2 * c, slots - 1)), :, sub(p)]
        from_up = chain[chain_dn(c, jnp.where(s == 0, 2 * high, slots - 1)), :, sub(p)]
        value = mine(me, p) + from_dn.astype(f32) + from_up.astype(f32)
        out[:, cols(s, p)] = (tok[:, cols(s, p)].astype(f32) + value).astype(bf16)
        value = (
            other[:, sub(p)].astype(f32)
            + cross[0, :, sub(p)].astype(f32)
            + cross[1, :, sub(p)].astype(f32)
        )
        out[:, cols(1 - s, p)] = (tok[:, cols(1 - s, p)].astype(f32) + value).astype(bf16)

    top = 1 - up

    def candidate(j, k):
        a = j - 1
        has_above = jnp.minimum(jnp.maximum(2 * high - a, 0), 1)
        has_below = jnp.minimum(jnp.maximum(2 * c - a, 0), 1)
        from_above = jnp.where(k == 0, 1 - top, 0)
        from_below = jnp.where(k == 0, top, 1 - top)
        later = from_above * has_above + from_below * has_below
        exists = jnp.where(j == 0, 1, later)
        slot = jnp.where(from_above == 1, gather_above(a), gather_below(a))
        return exists, jnp.where(j == 0, 2 * c + k, slot)

    def drain(j, carry):
        @pl.when(up > 0)
        def _():
            remote(
                blocks.at[0, :, side(s)], blocks.at[0, :, side(s)], up_send.at[j], up_recv.at[0, 0], above
            ).wait_send()

        @pl.when(dn > 0)
        def _():
            remote(
                blocks.at[0, :, side(s)], blocks.at[0, :, side(s)], dn_send.at[j], dn_recv.at[0, 0], below
            ).wait_send()

        return carry

    def drain_mate(image, carry):
        @pl.when(image // 2 != c)
        def _():
            from_mate(image).wait_send()

        return carry

    def tick(j, p):
        k = p // 2
        exists, slot = candidate(j, k)
        active = jnp.where(p < 4, exists, 0)

        @pl.when(active * (1 - p % 2) > 0)
        def _():
            @pl.when(j > 0)
            def _():
                from_mate(slot).wait_recv()

            project(slot)

        @pl.when(active * (p % 2) > 0)
        def _():
            attend()
            output(slot, k)

        last = jnp.where(j == slots - 1, 1, 0)

        @pl.when(jnp.where(j == 1, 1, 0) * jnp.where(p == 0, 1, 0) > 0)
        def _():
            share(0, mate).wait_recv()

            def one(q, carry):
                theirs[mate, :, sub(q)] = mine(mate, q).astype(bf16)
                return carry

            lax.fori_loop(0, pieces, one, 0)
            reveal().start()

        @pl.when(last * jnp.where(p == 0, 1, 0) > 0)
        def _():
            share(0, me).wait_recv()
            reveal().wait_recv()

            @pl.when(s == 0)
            def _():
                def one(q, carry):
                    finish(q)
                    return carry

                lax.fori_loop(0, pieces, one, 0)

        begin = jnp.where(p == 2, 1, 0) * jnp.minimum(j, 1) * (1 - last)

        @pl.when(begin * (1 - dn) * up > 0)
        def _():
            image = sum_into_up(c + 1, j + 1)
            share(0, image).wait_recv()

            def one(q, carry):
                theirs[image, :, sub(q)] = mine(image, q).astype(bf16)
                pass_up(image, j + 1, q)
                return carry

            lax.fori_loop(0, pieces, one, 0)

        @pl.when(begin * (1 - up) * dn > 0)
        def _():
            image = sum_into_dn(c - 1, j + 1)
            share(0, image).wait_recv()

            def one(q, carry):
                theirs[image, :, sub(q)] = mine(image, q).astype(bf16)
                pass_dn(image, j + 1, q)
                return carry

            lax.fori_loop(0, pieces, one, 0)

        @pl.when(dn > 0)
        def _():
            @pl.when(j < 2 * c)
            def _():
                image = gather_below(j)
                hop_up(image, j, p).wait_recv()

                @pl.when(up > 0)
                def _():
                    hop_up(image, j + 1, p).start()

                to_mate(image, p).start()

            @pl.when(j >= 2 * c)
            def _():
                image = sum_into_up(c, j)
                at = chain_up(c, j)

                @pl.when(image != mate)
                def _():
                    remote(
                        theirs.at[image, :, sub(p)],
                        chain.at[at, :, sub(p)],
                        up_send.at[j],
                        up_recv.at[j, p],
                        above,
                    ).wait_recv()

                @pl.when(image == me)
                def _():
                    add_cross_up(image, j, p).wait_recv()

                @pl.when(image >= 2 * c + 2)
                def _():
                    @pl.when(p == 0)
                    def _():
                        share(0, image).wait_recv()

                    theirs[image, :, sub(p)] = (
                        mine(image, p) + chain[at, :, sub(p)].astype(f32)
                    ).astype(bf16)
                    pass_up(image, j + 1, p)

        @pl.when(up > 0)
        def _():
            @pl.when(j < 2 * high)
            def _():
                image = gather_above(j)
                hop_dn(image, j, p).wait_recv()

                @pl.when(dn > 0)
                def _():
                    hop_dn(image, j + 1, p).start()

                to_mate(image, p).start()

            @pl.when(j >= 2 * high)
            def _():
                image = sum_into_dn(c, j)
                at = chain_dn(c, j)

                @pl.when(image != mate)
                def _():
                    remote(
                        theirs.at[image, :, sub(p)],
                        chain.at[at, :, sub(p)],
                        dn_send.at[j],
                        dn_recv.at[j, p],
                        below,
                    ).wait_recv()

                @pl.when(image == me)
                def _():
                    add_cross_dn(image, j, p).wait_recv()

                @pl.when(image < 2 * c)
                def _():
                    @pl.when(p == 0)
                    def _():
                        share(0, image).wait_recv()

                    theirs[image, :, sub(p)] = (
                        mine(image, p) + chain[at, :, sub(p)].astype(f32)
                    ).astype(bf16)
                    pass_dn(image, j + 1, p)

        @pl.when(up * jnp.where(p == 0, 1, 0) * jnp.where(j == 2 * c, 1, 0) > 0)
        def _():
            @pl.when(s == 0)
            def _():
                hop_up(2 * c + 1, 2 * c + 1, 0).start()

            for q in range(1, pieces):
                hop_up(2 * c + 1, 2 * c + 1, q).start()

        @pl.when(dn * jnp.where(p == 0, 1, 0) * jnp.where(j == 2 * high, 1, 0) > 0)
        def _():
            @pl.when(s == 0)
            def _():
                hop_dn(2 * c + 1, 2 * high + 1, 0).start()

            for q in range(1, pieces):
                hop_dn(2 * c + 1, 2 * high + 1, q).start()

        @pl.when(last * jnp.where(p == 1, 1, 0) > 0)
        def _():
            lax.fori_loop(0, slots - 1, drain, 0)
            lax.fori_loop(0, n, drain_mate, 0)
            reveal().wait_send()

        @pl.when(last * s > 0)
        def _():
            finish(p)

        for e, when in enumerate(times):
            @pl.when(j * pieces + p == when)
            def _():
                grad_event(e)

        @pl.when(p == pieces - 1)
        def _():
            for b in range(2):
                there, image = candidate(j, b)

                @pl.when(there > 0)
                def _():
                    share(b, image).wait_send()

    def slot_loop(j, carry):
        def piece_loop(p, inside):
            tick(j, p)
            return inside

        return lax.fori_loop(0, pieces, piece_loop, carry)

    lax.fori_loop(0, slots, slot_loop, 0)

    drain(slots - 1, 0)
    for h in range(2):
        for i in range(bits):
            scatter(h, i).wait_send()
            collect(h, i).wait_send()


def spread(mixed, total, mixed_hbm, total_hbm, wide, sem):
    parts = wide.shape[0]
    rows = wide.shape[1]
    first = pltpu.make_async_copy(mixed, mixed_hbm, sem.at[parts])
    first.start()

    def put(i):
        at = pl.ds(pl.multiple_of(i * rows, 8), rows)
        return pltpu.make_async_copy(wide.at[i], total_hbm.at[at, :], sem.at[i])

    def one(i, carry):
        at = pl.ds(pl.multiple_of(i * rows, 8), rows)
        wide[i, :, :] = total[at, :].astype(jnp.float32)
        put(i).start()
        return carry

    lax.fori_loop(0, parts, one, 0)

    def done(i, carry):
        put(i).wait()
        return carry

    lax.fori_loop(0, parts, done, 0)
    first.wait()


def body(n, groups, tokens, ln_gain, ln_bias, w_qkv, w_out, grad_partial):
    local_rows = tokens[0]
    rows, width = local_rows.shape
    inner = w_out.shape[0]
    grows = grad_partial.shape[1]
    chips = n // 2
    slots = 2 * chips
    bits = groups.bit_length() - 1
    half = width // 2
    pieces = pieces_of(half)
    dma = pltpu.SemaphoreType.DMA
    flops = 2 * rows * n * width * inner * 4
    vmem = pl.BlockSpec(memory_space=pltpu.VMEM)
    hbm = pl.BlockSpec(memory_space=pl.ANY)
    bf16 = jnp.bfloat16
    results = (rows + grows) * width * 2
    income = sum(grows >> (i + 2) for i in range(bits))
    mixed, total = pl.pallas_call(
        functools.partial(kernel, n, groups),
        out_shape=(pltpu.VMEM((rows, width), bf16), pltpu.VMEM((grows, width), bf16)),
        in_specs=[hbm, vmem, vmem, hbm, hbm, hbm],
        out_specs=(vmem, vmem),
        scratch_shapes=[
            pltpu.VMEM((3, width, inner), bf16),
            pltpu.VMEM((inner, width), bf16),
            pltpu.VMEM((rows, width), bf16),
            pltpu.VMEM((n, rows, width), bf16),
            pltpu.VMEM((n, rows, half), bf16),
            pltpu.VMEM((2, rows, half), bf16),
            pltpu.VMEM((slots + 2, rows, half), bf16),
            pltpu.VMEM((2, rows, half), bf16),
            pltpu.VMEM((rows, half), bf16),
            pltpu.VMEM((3, rows, inner), bf16),
            pltpu.VMEM((rows, inner), bf16),
            pltpu.VMEM((2, income, width), bf16),
            dma((5,)),
            dma((pieces + 1,)),
            dma((pieces + 1,)),
            dma((slots,)),
            dma((slots, pieces)),
            dma((slots,)),
            dma((slots, pieces)),
            dma((n,)),
            dma((n,)),
            dma((2,)),
            dma((n,)),
            dma((1,)),
            dma((1,)),
            dma((pieces,)),
            dma((pieces,)),
            dma((2, bits)),
            dma((2, bits)),
            dma((2, bits)),
            dma((2, bits)),
        ],
        compiler_params=pltpu.CompilerParams(
            collective_id=0, has_side_effects=True, vmem_limit_bytes=66_900_000 - results
        ),
        cost_estimate=pl.CostEstimate(
            flops=flops * 8, bytes_accessed=300_000_000, transcendentals=0
        ),
    )(
        local_rows,
        ln_gain.reshape(1, width),
        ln_bias.reshape(1, width),
        jnp.transpose(w_qkv, (1, 0, 2)),
        w_out,
        grad_partial[0],
    )
    parts = grows // 64
    mixed, grad_sum = pl.pallas_call(
        spread,
        out_shape=(
            jax.ShapeDtypeStruct((rows, width), bf16),
            jax.ShapeDtypeStruct((grows, width), jnp.float32),
        ),
        in_specs=[vmem, vmem],
        out_specs=(hbm, hbm),
        scratch_shapes=[
            pltpu.VMEM((parts, grows // parts, width), jnp.float32),
            dma((parts + 1,)),
        ],
        compiler_params=pltpu.CompilerParams(vmem_limit_bytes=grows * width * 4 + 2_000_000),
        cost_estimate=pl.CostEstimate(
            flops=grows * width, bytes_accessed=grows * width * 6, transcendentals=0
        ),
    )(mixed, total)
    return (mixed[None], grad_sum)


def solution(mesh):
    placed = (
        P("dp", "mp", None),
        P(),
        P(),
        P(None, None, "mp"),
        P("mp", None),
        P("dp", "mp", None),
    )
    return jax.shard_map(
        functools.partial(body, mesh.shape["mp"], mesh.shape["dp"]),
        mesh=mesh,
        in_specs=placed,
        out_specs=(P("dp", "mp", None), P("mp", None)),
        check_vma=False,
    )
```
